128 devices in a mesh: gx: 8 (over y, core), gy: 16 (over z, x).
Axes of the slice: x: 4, y: 4, z: 4, core: 2. Of those that a mesh axis runs over, the one named last changes fastest.
Arguments:
- forcing: float32 [16, 512, 2048], P(None, 'gy', 'gx'), may hold values from -6 to 6
- damping: float32 [16, 512, 2048], P(None, 'gy', 'gx'), may hold values from 0.5 to 4
- coupling: float32 [16, 16], replicated, may hold values from -1.5 to 1.5
- wind_lon: float32 [512, 2048], P('gy', 'gx'), may hold values from -0.5 to 0.5
- wind_lat: float32 [512, 2048], P('gy', 'gx'), may hold values from -0.5 to 0.5
Outputs:
- solution: float32 [16, 512, 2048], P(None, 'gy', 'gx')
- residual: float32 [16, 512, 2048], P(None, 'gy', 'gx')
The draws below stay inside these ranges and needn't reach their ends.
All inputs are finite; a program needn't handle non-finite values.
Results may differ from the reference program's by a relative error of at most 0.0003.
Values sent between devices are 32-bit elements; how exact they have to be, the bound alone decides.
No kernel may reach another device: no remote copies, remote signals or barrier semaphores. Data moves between devices by JAX's collectives and lax.ppermute only.
A program may use at most 64 MiB of HBM per device.

```python
import math
import jax
import jax.numpy as jnp
from jax import lax

CH = 16
ITERS = 8
NLAT = 512
NLON = 2048


def block_scale(stream_key, dims, cuts, smallest, high):
    def one(position, parts):
        steps = jax.random.uniform(jax.random.fold_in(jax.random.fold_in(stream_key, 6), position), (parts,), jnp.float32, smallest / len(cuts), high / len(cuts))
        return jnp.repeat(jnp.exp(steps), dims[position] // parts).reshape((-1,) + (1,) * (len(dims) - position - 1))

    factor_of = one(*cuts[0])
    for cut in cuts[1:]:
        factor_of = factor_of * one(*cut)
    return factor_of


def scatter_about(own_key, extent, scale, limit, pieces=(), held_as=jnp.bfloat16):
    factor_of = block_scale(own_key, extent, pieces, -0.22, 0.18) if pieces else 1.0
    drawn = jax.random.normal(own_key, extent, jnp.float32) * scale * factor_of
    return jnp.minimum(jnp.maximum(drawn, -limit), limit).astype(held_as)


def setup_inputs(seed: int = 0) -> dict:
    seeds = jax.random.split(jax.random.key(seed), 6)
    return {
        "forcing": scatter_about(seeds[0], (CH, NLAT, NLON), 1.0, 6.0, ((1, 16), (2, 8)), jnp.float32),
        "damping": jnp.clip(jnp.exp(math.log(4.0) - 2.0794415 * jax.random.uniform(seeds[1], (CH, NLAT, NLON), jnp.float32) ** block_scale(seeds[1], (CH, NLAT, NLON), ((1, 16), (2, 8)), -0.2, 0.2)), 0.5, 4.0),
        "coupling": scatter_about(seeds[2], (CH, CH), CH ** -0.5, 1.5, (), jnp.float32),
        "wind_lon": jnp.clip(jax.random.uniform(seeds[3], (NLAT, NLON), jnp.float32, -0.5, 0.5) * block_scale(seeds[3], (NLAT, NLON), ((0, 16), (1, 8)), -0.4, 0.0), -0.5, 0.5),
        "wind_lat": jnp.clip(jax.random.uniform(seeds[4], (NLAT, NLON), jnp.float32, -0.5, 0.5) * block_scale(seeds[4], (NLAT, NLON), ((0, 16), (1, 8)), -0.4, 0.0), -0.5, 0.5),
    }


COUPLE = 0.25
DIFF_LAT = 0.5
DIFF_LON = 0.5
GUARD = 1.0

def apply_core(padded, damping, coupling, wind_lon, wind_lat, diffuse_lon):
    centre = padded[:, 2:-2, 2:-2]
    east_one = padded[:, 2:-2, 3:-1]
    west_one = padded[:, 2:-2, 1:-3]
    east_two = padded[:, 2:-2, 4:]
    west_two = padded[:, 2:-2, :-4]
    north_one = padded[:, 3:-1, 2:-2]
    south_one = padded[:, 1:-3, 2:-2]
    north_two = padded[:, 4:, 2:-2]
    south_two = padded[:, :-4, 2:-2]
    slope_lon = (8.0 * (east_one - west_one) - (east_two - west_two)) / 12.0
    slope_lat = (8.0 * (north_one - south_one) - (north_two - south_two)) / 12.0
    coupled = COUPLE * jnp.einsum('ij,jab->iab', coupling, centre, precision=lax.Precision.HIGHEST)
    return (1.0 + damping) * centre + coupled + diffuse_lon * (2.0 * centre - east_one - west_one) + DIFF_LAT * (2.0 * centre - north_one - south_one) + wind_lon * slope_lon + wind_lat * slope_lat

def lon_diffusion(row_pos, lat_total):
    phi = -math.pi / 2 + (row_pos + 0.5) * (math.pi / lat_total)
    return DIFF_LON / (jnp.cos(phi) ** 2 + 0.1)

def operate(source, damping, coupling, wind_lon, wind_lat):
    padded = jnp.pad(source, ((0, 0), (2, 2), (0, 0)))
    padded = jnp.concatenate([padded[:, :, -2:], padded, padded[:, :, :2]], axis=2)
    row_pos = jnp.arange(NLAT).astype(jnp.float32)
    diffuse = lon_diffusion(row_pos, NLAT)[:, None]
    return apply_core(padded, damping, coupling, wind_lon, wind_lat, diffuse)

def least_squares(heights, first):
    num_steps = heights.shape[1]
    target = jnp.zeros((num_steps + 1,), jnp.float32).at[0].set(first)
    rotated = heights
    cosines = []
    sines = []
    for column in range(num_steps):
        column_vec = rotated[:, column]
        for earlier in range(column):
            upper_val = column_vec[earlier]
            lower_val = column_vec[earlier + 1]
            column_vec = column_vec.at[earlier].set(cosines[earlier] * upper_val + sines[earlier] * lower_val)
            column_vec = column_vec.at[earlier + 1].set(-sines[earlier] * upper_val + cosines[earlier] * lower_val)
        upper_val = column_vec[column]
        lower_val = column_vec[column + 1]
        radius = jnp.sqrt(upper_val * upper_val + lower_val * lower_val)
        cosine = upper_val / radius
        sine_val = lower_val / radius
        column_vec = column_vec.at[column].set(radius).at[column + 1].set(0.0)
        rotated = rotated.at[:, column].set(column_vec)
        upper_val = target[column]
        lower_val = target[column + 1]
        target = target.at[column].set(cosine * upper_val + sine_val * lower_val)
        target = target.at[column + 1].set(-sine_val * upper_val + cosine * lower_val)
        cosines.append(cosine)
        sines.append(sine_val)
    weights = [None] * num_steps
    for column in reversed(range(num_steps)):
        partial_value = target[column]
        for later_col in range(column + 1, num_steps):
            partial_value = partial_value - rotated[column, later_col] * weights[later_col]
        weights[column] = partial_value / rotated[column, column]
    return weights

def reference(forcing, damping, coupling, wind_lon, wind_lat):
    scale_first = jnp.sqrt(jnp.sum(forcing * forcing) + GUARD)
    krylov = [forcing / scale_first]
    heights = jnp.zeros((ITERS + 1, ITERS), jnp.float32)
    for column in range(ITERS):
        applied = operate(krylov[column], damping, coupling, wind_lon, wind_lat)
        coeffs = jnp.stack([jnp.sum(vector * applied) for vector in krylov])
        for earlier in range(len(krylov)):
            applied = applied - coeffs[earlier] * krylov[earlier]
        subdiag = jnp.sqrt(jnp.sum(applied * applied) + GUARD)
        heights = heights.at[:column + 1, column].set(coeffs).at[column + 1, column].set(subdiag)
        if column + 1 < ITERS:
            krylov.append(applied / subdiag)
    weights = least_squares(heights, scale_first)
    solution = weights[0] * krylov[0]
    for column in range(1, ITERS):
        solution = solution + weights[column] * krylov[column]
    residual = forcing - operate(solution, damping, coupling, wind_lon, wind_lat)
    return (solution, residual)
```

```python
import functools
import math

import jax
import jax.numpy as jnp
import numpy as np
from jax import lax
from jax.experimental import pallas as pl
from jax.experimental.pallas import tpu as pltpu
from jax.sharding import PartitionSpec as P

ITERS = 8
CH = 16
ROWS = 32
COLS = 256
RIM = 2 * ITERS
EXT_ROWS = ROWS + 2 * RIM
EXT_COLS = COLS + 128
COUPLE = 0.25
DIFF_LAT = 0.5
DIFF_LON = 0.5
GUARD = 1.0

LOW, HIGH = 1.5, 26.0
CENTRE = (LOW + HIGH) / 2
SCALE = 4.0 / (HIGH - LOW)
NUM = ITERS + 1
PAIRS = [(i, j) for j in range(NUM) for i in range(j + 1)]
F32 = jnp.float32


def pack_kernel(f_ref, d_ref, wl_ref, wt_ref, s1_ref, s2_ref, x1_ref, x2_ref):
    par_y = lax.rem(lax.axis_index("gy"), 2)
    par_x = lax.rem(lax.axis_index("gx"), 2)
    for ref, half in ((s1_ref, 1 - par_y), (s2_ref, par_y)):
        for q in range(2):
            off = pl.multiple_of(half * 16 + 8 * q, 8)
            for src, base in ((f_ref, 0), (d_ref, 16)):
                for c in range(2):
                    ref[base + 8 * q : base + 8 * q + 8, 8 * c : 8 * c + 8, :] = jnp.swapaxes(
                        src[8 * c : 8 * c + 8, pl.ds(off, 8), :], 0, 1
                    )
        off = pl.multiple_of(half * 16, 16)
        ref[32] = wl_ref[pl.ds(off, 16), :]
        ref[33] = wt_ref[pl.ds(off, 16), :]
    group = lax.broadcasted_iota(jnp.int32, (8, 128), 1) // 16

    def gather(tiles):
        left = jnp.zeros((8, 128), F32)
        right = jnp.zeros((8, 128), F32)
        for g, (low, high) in enumerate(tiles):
            left = jnp.where(group == g, pltpu.roll(low, 16 * g, 1) if g else low, left)
            shift = (16 * g + 16) % 128
            right = jnp.where(group == g, pltpu.roll(high, shift, 1) if shift else high, right)
        return jnp.where(par_x == 0, right, left), jnp.where(par_x == 0, left, right)

    winds = gather(
        [
            (ref[8 * q : 8 * q + 8, :128], ref[8 * q : 8 * q + 8, 128:])
            for ref in (wl_ref, wt_ref)
            for q in range(4)
        ]
    )
    for half in range(2):
        slot = 0
        for base in (0, 16):
            for q in range(2):
                for c in range(2):
                    tiles = []
                    for g in range(8):
                        row = base + 8 * q + g
                        pick = []
                        for t in range(2):
                            one = s1_ref[row, 8 * c : 8 * c + 8, 128 * t : 128 * t + 128]
                            two = s2_ref[row, 8 * c : 8 * c + 8, 128 * t : 128 * t + 128]
                            pick.append(jnp.where(par_y == half, two, one))
                        tiles.append(tuple(pick))
                    first, second = gather(tiles)
                    x1_ref[half, 8 * slot : 8 * slot + 8, :] = first
                    x2_ref[half, 8 * slot : 8 * slot + 8, :] = second
                    slot += 1
        x1_ref[half, 64:72, :] = winds[0]
        x2_ref[half, 64:72, :] = winds[1]


def main_kernel(
    s1_ref, s2_ref, r1_ref, r2_ref, g1_ref, g2_ref, c1_ref, c2_ref, tab_ref, kron_ref,
    out_ref, gram_ref,
    p_ref, d_ref, w_ref, k_ref, coef_ref, sums_ref, in_sem, out_sem,
):
    par_y = lax.rem(lax.axis_index("gy"), 2)
    par_x = lax.rem(lax.axis_index("gx"), 2)
    copies = []

    def fetch(src, dst):
        copy = pltpu.make_async_copy(src, dst, in_sem.at[len(copies)])
        copy.start()
        copies.append(copy)

    start = pl.multiple_of(lax.axis_index("gy") * ROWS, ROWS)
    fetch(tab_ref.at[pl.ds(start, EXT_ROWS)], k_ref)
    dest = ((s1_ref, 32 - 16 * par_y), (s2_ref, 16 + 16 * par_y), (r1_ref, 48 - 48 * par_y), (r2_ref, 48 * par_y))
    for src, row in dest:
        row = pl.multiple_of(row, 16)
        fetch(src.at[0:16], p_ref.at[0, pl.ds(row, 16), :, pl.ds(0, COLS)])
        fetch(src.at[16:32], d_ref.at[pl.ds(row, 16), :, pl.ds(0, COLS)])
        fetch(src.at[32:34], w_ref.at[:, pl.ds(row, 16), pl.ds(0, COLS)])

    lane = lax.broadcasted_iota(jnp.int32, (8, 128), 1)

    def spread(east, west, g):
        e = pltpu.roll(east, (128 - 16 * g) % 128, 1) if g else east
        shift = (112 - 16 * g) % 128
        w = pltpu.roll(west, shift, 1) if shift else west
        return jnp.where(lane < 16, e, jnp.where(lane >= 112, w, 0.0))

    places = (
        (lambda sl: g1_ref[0, sl], lambda sl: g2_ref[0, sl], 16, 0),
        (lambda sl: g1_ref[1, sl], lambda sl: g2_ref[1, sl], 32, 1),
        (lambda sl: c1_ref[0, sl], lambda sl: c1_ref[1, sl], 48 - 48 * par_y, par_y),
        (lambda sl: c2_ref[0, sl], lambda sl: c2_ref[1, sl], 48 * par_y, 1 - par_y),
    )
    for one, two, row, half in places:
        slot = 0
        for ref in (p_ref.at[0], d_ref):
            for q in range(2):
                for c in range(2):
                    a = one(slice(8 * slot, 8 * slot + 8))
                    b = two(slice(8 * slot, 8 * slot + 8))
                    east = jnp.where(par_x == 0, a, b)
                    west = jnp.where(par_x == 0, b, a)
                    for g in range(8):
                        ref[row + 8 * q + g, 8 * c : 8 * c + 8, COLS:] = spread(east, west, g)
                    slot += 1
        a = one(slice(64, 72))
        b = two(slice(64, 72))
        east = jnp.where(par_x == 0, a, b)
        west = jnp.where(par_x == 0, b, a)
        for field in range(2):
            for q in range(2):
                low = spread(east, west, 4 * field + q)
                high = spread(east, west, 4 * field + 2 + q)
                tile = jnp.where(half == 0, low, high)
                w_ref[field, pl.ds(pl.multiple_of(row + 8 * q, 8), 8), COLS:] = tile

    kron = kron_ref[...]
    kron_hi = kron.astype(jnp.bfloat16)
    kron_lo = (kron - kron_hi.astype(F32)).astype(jnp.bfloat16)
    for copy in copies:
        copy.wait()

    for q in range(EXT_ROWS // 8):
        rows = slice(8 * q, 8 * q + 8)
        diffuse = jnp.concatenate([k_ref[rows]] * 3, axis=1)
        live = jnp.where(diffuse > 0.0, 1.0, 0.0)
        lon = w_ref[0, rows] * (live * (SCALE / 12.0))
        lat = w_ref[1, rows] * (live * (SCALE / 12.0))
        kx = diffuse * SCALE
        half_lat = live * (SCALE * DIFF_LAT)
        coef_ref[0, rows] = 8.0 * lon - kx
        coef_ref[1, rows] = -8.0 * lon - kx
        coef_ref[2, rows] = -lon
        coef_ref[3, rows] = 8.0 * lat - half_lat
        coef_ref[4, rows] = -8.0 * lat - half_lat
        coef_ref[5, rows] = -lat
        coef_ref[6, rows] = live * (SCALE * (1.0 + 2.0 * DIFF_LAT - CENTRE)) + 2.0 * kx
        coef_ref[7, rows] = live * SCALE

    @pl.loop(0, EXT_ROWS, unroll=2)
    def _(r):
        d_ref[r] = d_ref[r] * coef_ref[7, pl.ds(r, 1)] + coef_ref[6, pl.ds(r, 1)]

    outs = []

    def emit(step):
        copy = pltpu.make_async_copy(
            p_ref.at[step, pl.ds(RIM, ROWS), :, pl.ds(0, COLS)], out_ref.at[step], out_sem.at[step]
        )
        copy.start()
        outs.append(copy)

    emit(0)
    for step in range(1, NUM):
        low = 2 * step
        blocks = (EXT_ROWS - 2 * low + 7) // 8

        @pl.loop(0, blocks)
        def _(block, step=step, low=low):
            r0 = jnp.minimum(low + 8 * block, EXT_ROWS - low - 8)
            flat = p_ref[step - 1, pl.ds(r0, 8)].reshape(8 * CH, EXT_COLS)
            hi = flat.astype(jnp.bfloat16)
            lo = (flat - hi.astype(F32)).astype(jnp.bfloat16)
            mixed = jnp.dot(kron_hi, hi, preferred_element_type=F32)
            mixed = mixed + jnp.dot(kron_hi, lo, preferred_element_type=F32)
            mixed = mixed + jnp.dot(kron_lo, hi, preferred_element_type=F32)
            mixed = mixed.reshape(8, CH, EXT_COLS)
            for i in range(8):
                r = r0 + i
                c = p_ref[step - 1, r]
                acc = mixed[i] + d_ref[r] * c
                if step > 1:
                    acc = acc - p_ref[step - 2, r]
                coef = [coef_ref[k, pl.ds(r, 1)] for k in range(6)]
                acc = acc + coef[0] * pltpu.roll(c, EXT_COLS - 1, 1)
                acc = acc + coef[1] * pltpu.roll(c, 1, 1)
                acc = acc + coef[2] * (pltpu.roll(c, EXT_COLS - 2, 1) - pltpu.roll(c, 2, 1))
                acc = acc + coef[3] * p_ref[step - 1, r + 1]
                acc = acc + coef[4] * p_ref[step - 1, r - 1]
                acc = acc + coef[5] * (p_ref[step - 1, r + 2] - p_ref[step - 1, r - 2])
                p_ref[step, r] = acc

        emit(step)

    sums_ref[...] = jnp.zeros_like(sums_ref)
    for lo_k, hi_k in ((0, 6), (6, NUM)):
        pairs = [(n, i, j) for n, (i, j) in enumerate(PAIRS) if lo_k <= j < hi_k]

        def body(r, accs, pairs=pairs, hi_k=hi_k):
            accs = list(accs)
            for c in range(2):
                for t in range(2):
                    vecs = [
                        p_ref[k, RIM + r, 8 * c : 8 * c + 8, 128 * t : 128 * t + 128]
                        for k in range(hi_k)
                    ]
                    for n, (_, i, j) in enumerate(pairs):
                        accs[n] = accs[n] + vecs[i] * vecs[j]
            return tuple(accs)

        accs = lax.fori_loop(0, ROWS, body, tuple(jnp.zeros((8, 128), F32) for _ in pairs))
        for (n, _, _), acc in zip(pairs, accs):
            sums_ref[n : n + 1, :] = jnp.sum(acc, axis=0, keepdims=True)
    gram = lax.dot_general(
        jnp.ones((128, 128), F32), sums_ref[...], (((1,), (1,)), ((), ())),
        precision=lax.Precision.HIGHEST, preferred_element_type=F32,
    )
    gram_ref[...] = gram
    for copy in outs:
        copy.wait()


def small_solve(gram):
    inv = 1.0 / SCALE

    def total(values):
        values = list(values)
        while len(values) > 1:
            nxt = [values[k] + values[k + 1] for k in range(0, len(values) - 1, 2)]
            if len(values) % 2:
                nxt.append(values[-1])
            values = nxt
        return values[0]

    def shifted(vec):
        out = []
        for k in range(len(vec) + 1):
            terms = [vec[m] for m in (k - 1, k + 1) if 0 <= m < len(vec)]
            parts = [total(terms) * inv] if terms else []
            if k < len(vec):
                parts.append(vec[k] * CENTRE)
            out.append(total(parts))
        return out

    def dot(one, two):
        return total(x * y for x, y in zip(one, two))

    first = jnp.sqrt(gram[0][0] + GUARD)
    inv_first = 1.0 / first
    basis = [[inv_first]]
    images = [[gram[k][0] * inv_first for k in range(NUM)]]
    cosines, sines, upper = [], [], []
    target = [first]
    for col in range(ITERS):
        work = shifted(basis[col])
        image = [dot(work, gram[k]) for k in range(NUM)]
        coeffs = [dot(basis[i], image) for i in range(col + 1)]
        work = [
            total([work[k]] + [-(coeffs[i] * basis[i][k]) for i in range(col + 1) if k < len(basis[i])])
            for k in range(len(work))
        ]
        image = [total([image[k]] + [-(coeffs[i] * images[i][k]) for i in range(col + 1)]) for k in range(NUM)]
        subdiag = jnp.sqrt(jnp.maximum(dot(work, image), 0.0) + GUARD)
        if col + 1 < ITERS:
            scale = 1.0 / subdiag
            basis.append([x * scale for x in work])
            images.append([x * scale for x in image])
        column = list(coeffs)
        for k in range(col):
            a, b = column[k], column[k + 1]
            column[k] = cosines[k] * a + sines[k] * b
            column[k + 1] = cosines[k] * b - sines[k] * a
        a, b = column[col], subdiag
        radius = jnp.sqrt(a * a + b * b)
        inv_radius = 1.0 / radius
        cosines.append(a * inv_radius)
        sines.append(b * inv_radius)
        column[col] = radius
        upper.append((column, inv_radius))
        last = target[col]
        target[col] = cosines[col] * last
        target.append(-(sines[col] * last))
    weights = [None] * ITERS
    for col in reversed(range(ITERS)):
        rest = [target[col]] + [-(upper[k][0][col] * weights[k]) for k in range(col + 1, ITERS)]
        weights[col] = total(rest) * upper[col][1]
    coef = [total([weights[j] * basis[j][k] for j in range(k, ITERS)]) for k in range(ITERS)]
    return coef, shifted(coef)


def final_kernel(p_ref, rows_ref, x_ref, r_ref, work_ref):
    summed = jnp.sum(rows_ref[...], axis=0, keepdims=True)
    gram = [[None] * NUM for _ in range(NUM)]
    for n, (i, j) in enumerate(PAIRS):
        gram[i][j] = gram[j][i] = jnp.broadcast_to(summed[:, n : n + 1], (8, 128))
    coef, image = small_solve(gram)
    for k in range(ITERS):
        work_ref[k] = coef[k]
    work_ref[ITERS] = 1.0 - image[0]
    for k in range(1, NUM):
        work_ref[ITERS + k] = -image[k]

    @pl.loop(0, ROWS // 8)
    def _(b):
        off = pl.multiple_of(b * 8, 8)
        for c in range(2):
            for t in range(2):
                xs = rs = None
                for k in range(NUM):
                    vec = p_ref[k, pl.ds(off, 8), 8 * c : 8 * c + 8, 128 * t : 128 * t + 128]
                    part = vec * work_ref[ITERS + k]
                    rs = part if rs is None else rs + part
                    if k < ITERS:
                        part = vec * work_ref[k]
                        xs = part if xs is None else xs + part
                where = (slice(8 * c, 8 * c + 8), pl.ds(off, 8), slice(128 * t, 128 * t + 128))
                x_ref[where] = jnp.swapaxes(xs, 0, 1)
                r_ref[where] = jnp.swapaxes(rs, 0, 1)


def diffusion_table(lat_total):
    row = np.arange(-RIM, lat_total + RIM, dtype=np.float64)
    phi = -math.pi / 2 + (row + 0.5) * (math.pi / lat_total)
    kx = DIFF_LON / (np.cos(phi) ** 2 + 0.1)
    kx = np.where((row >= 0) & (row < lat_total), kx, 0.0)
    return np.repeat(kx[:, None], 128, axis=1).astype(np.float32)


VMEM = pl.BlockSpec(memory_space=pltpu.VMEM)
ANY = pl.BlockSpec(memory_space=pl.ANY)


def shape(*dims):
    return jax.ShapeDtypeStruct(dims, F32)


def pairing(count, odd, closed):
    pairs = []
    for i in range(count):
        partner = i + 1 if (i % 2 == 0) != odd else i - 1
        if closed:
            partner %= count
        if 0 <= partner < count:
            pairs.append((i, partner))
    return pairs


def per_device(forcing, damping, coupling, wind_lon, wind_lat, *, nx, ny):
    s1, s2, x1, x2 = pl.pallas_call(
        pack_kernel,
        in_specs=[VMEM] * 4,
        out_specs=[VMEM] * 4,
        out_shape=[shape(34, 16, COLS)] * 2 + [shape(2, 72, 128)] * 2,
        name="pack",
    )(forcing, damping, wind_lon, wind_lat)
    g1 = lax.ppermute(x1, "gx", pairing(nx, False, True))
    g2 = lax.ppermute(x2, "gx", pairing(nx, True, True))
    r1 = lax.ppermute(s1, "gy", pairing(ny, False, False))
    r2 = lax.ppermute(s2, "gy", pairing(ny, True, False))
    both = jnp.stack([g1, g2])
    par_y = lax.rem(lax.axis_index("gy"), 2)
    k1 = lax.dynamic_index_in_dim(both, 1 - par_y, 1, keepdims=False)
    k2 = lax.dynamic_index_in_dim(both, par_y, 1, keepdims=False)
    c1 = lax.ppermute(k1, "gy", pairing(ny, False, False))
    c2 = lax.ppermute(k2, "gy", pairing(ny, True, False))
    table = jnp.asarray(diffusion_table(ny * ROWS))
    kron = jnp.kron(jnp.eye(8, dtype=F32), coupling * (COUPLE * SCALE))
    basis, gram = pl.pallas_call(
        main_kernel,
        in_specs=[ANY] * 4 + [VMEM] * 4 + [ANY, VMEM],
        out_specs=[ANY, VMEM],
        out_shape=[shape(NUM, ROWS, CH, COLS), shape(128, 128)],
        scratch_shapes=[
            pltpu.VMEM((NUM, EXT_ROWS, CH, EXT_COLS), F32),
            pltpu.VMEM((EXT_ROWS, CH, EXT_COLS), F32),
            pltpu.VMEM((2, EXT_ROWS, EXT_COLS), F32),
            pltpu.VMEM((EXT_ROWS, 128), F32),
            pltpu.VMEM((8, EXT_ROWS, EXT_COLS), F32),
            pltpu.VMEM((128, 128), F32),
            pltpu.SemaphoreType.DMA((13,)),
            pltpu.SemaphoreType.DMA((NUM,)),
        ],
        compiler_params=pltpu.CompilerParams(vmem_limit_bytes=40 * 2**20),
        name="powers",
    )(s1, s2, r1, r2, g1, g2, c1, c2, table, kron)
    rows = lax.all_to_all(gram, ("gx", "gy"), 0, 0, tiled=True)
    return pl.pallas_call(
        final_kernel,
        in_specs=[VMEM, VMEM],
        out_specs=[VMEM, VMEM],
        out_shape=[shape(CH, ROWS, COLS)] * 2,
        scratch_shapes=[pltpu.VMEM((ITERS + NUM, 8, 128), F32)],
        name="finish",
    )(basis, rows)


def solution(mesh):
    spec = P(None, "gy", "gx")
    flat = P("gy", "gx")
    return jax.shard_map(
        functools.partial(per_device, nx=mesh.shape["gx"], ny=mesh.shape["gy"]),
        mesh=mesh,
        in_specs=(spec, spec, P(), flat, flat),
        out_specs=(spec, spec),
        check_vma=False,
    )
```

```python
import functools
import math

import jax
import jax.numpy as jnp
import numpy as np
from jax import lax
from jax.experimental import pallas as pl
from jax.experimental.pallas import tpu as pltpu
from jax.sharding import PartitionSpec as P

ITERS = 8
CH = 16
ROWS = 32
COLS = 256
RIM = 2 * ITERS
EXT_ROWS = ROWS + 2 * RIM
EXT_COLS = COLS + 128
COUPLE = 0.25
DIFF_LAT = 0.5
DIFF_LON = 0.5
GUARD = 1.0

LOW, HIGH = 1.5, 26.0
CENTRE = (LOW + HIGH) / 2
SCALE = 4.0 / (HIGH - LOW)
NUM = ITERS + 1
PAIRS = [(i, j) for j in range(NUM) for i in range(j + 1)]
F32 = jnp.float32


def pack_kernel(f_ref, d_ref, wl_ref, wt_ref, s1_ref, s2_ref, x1_ref, x2_ref):
    par_y = lax.rem(lax.axis_index("gy"), 2)
    par_x = lax.rem(lax.axis_index("gx"), 2)
    for ref, half in ((s1_ref, 1 - par_y), (s2_ref, par_y)):
        for q in range(2):
            off = pl.multiple_of(half * 16 + 8 * q, 8)
            for src, base in ((f_ref, 0), (d_ref, 16)):
                for c in range(2):
                    ref[base + 8 * q : base + 8 * q + 8, 8 * c : 8 * c + 8, :] = jnp.swapaxes(
                        src[8 * c : 8 * c + 8, pl.ds(off, 8), :], 0, 1
                    )
        off = pl.multiple_of(half * 16, 16)
        ref[32] = wl_ref[pl.ds(off, 16), :]
        ref[33] = wt_ref[pl.ds(off, 16), :]
    group = lax.broadcasted_iota(jnp.int32, (8, 128), 1) // 16

    def gather(tiles):
        left = jnp.zeros((8, 128), F32)
        right = jnp.zeros((8, 128), F32)
        for g, (low, high) in enumerate(tiles):
            left = jnp.where(group == g, pltpu.roll(low, 16 * g, 1) if g else low, left)
            shift = (16 * g + 16) % 128
            right = jnp.where(group == g, pltpu.roll(high, shift, 1) if shift else high, right)
        return jnp.where(par_x == 0, right, left), jnp.where(par_x == 0, left, right)

    winds = gather(
        [
            (ref[8 * q : 8 * q + 8, :128], ref[8 * q : 8 * q + 8, 128:])
            for ref in (wl_ref, wt_ref)
            for q in range(4)
        ]
    )
    for half in range(2):
        slot = 0
        for base in (0, 16):
            for q in range(2):
                for c in range(2):
                    tiles = []
                    for g in range(8):
                        row = base + 8 * q + g
                        pick = []
                        for t in range(2):
                            one = s1_ref[row, 8 * c : 8 * c + 8, 128 * t : 128 * t + 128]
                            two = s2_ref[row, 8 * c : 8 * c + 8, 128 * t : 128 * t + 128]
                            pick.append(jnp.where(par_y == half, two, one))
                        tiles.append(tuple(pick))
                    first, second = gather(tiles)
                    x1_ref[half, 8 * slot : 8 * slot + 8, :] = first
                    x2_ref[half, 8 * slot : 8 * slot + 8, :] = second
                    slot += 1
        x1_ref[half, 64:72, :] = winds[0]
        x2_ref[half, 64:72, :] = winds[1]


LANE_SHAPE = (8, 128)


def place_half(src_ref, one, two, row, half, p0_ref, d_ref, coef_ref, k_ref):
    par_x = lax.rem(lax.axis_index("gx"), 2)
    lane = lax.broadcasted_iota(jnp.int32, LANE_SHAPE, 1)
    row = pl.multiple_of(row, 16)

    def spread(east, west, g):
        e = pltpu.roll(east, (128 - 16 * g) % 128, 1) if g else east
        shift = (112 - 16 * g) % 128
        w = pltpu.roll(west, shift, 1) if shift else west
        return jnp.where(lane < 16, e, jnp.where(lane >= 112, w, 0.0))

    def sides(slot):
        a = one(slice(8 * slot, 8 * slot + 8))
        b = two(slice(8 * slot, 8 * slot + 8))
        return jnp.where(par_x == 0, a, b), jnp.where(par_x == 0, b, a)

    east, west = sides(8)
    scales = []
    for q in range(2):
        rows = pl.ds(pl.multiple_of(row + 8 * q, 8), 8)
        k = k_ref[rows]
        live = jnp.where(k > 0.0, 1.0, 0.0)
        kx = k * SCALE
        half_lat = live * (SCALE * DIFF_LAT)
        fixed = live * (SCALE * (1.0 + 2.0 * DIFF_LAT - CENTRE)) + 2.0 * kx
        for t in range(3):
            lanes = slice(128 * t, 128 * t + 128)
            winds = []
            for field in range(2):
                if t < 2:
                    wind = src_ref[32 + field, 8 * q : 8 * q + 8, lanes]
                else:
                    low = spread(east, west, 4 * field + q)
                    high = spread(east, west, 4 * field + 2 + q)
                    wind = jnp.where(half == 0, low, high)
                winds.append(wind * (live * (SCALE / 12.0)))
            lon, lat = winds
            coef_ref[0, rows, lanes] = 8.0 * lon - kx
            coef_ref[1, rows, lanes] = -8.0 * lon - kx
            coef_ref[2, rows, lanes] = -lon
            coef_ref[3, rows, lanes] = 8.0 * lat - half_lat
            coef_ref[4, rows, lanes] = -8.0 * lat - half_lat
            coef_ref[5, rows, lanes] = -lat
        scales.append((live * SCALE, fixed))
    for q in range(2):
        for c in range(2):
            subs = slice(8 * c, 8 * c + 8)
            fe, fw = sides(2 * q + c)
            de, dw = sides(4 + 2 * q + c)
            for g in range(8):
                r = 8 * q + g
                p0_ref[row + r, subs, :COLS] = src_ref[r, subs]
                p0_ref[row + r, subs, COLS:] = spread(fe, fw, g)
                mul, add = (x[g : g + 1] for x in scales[q])
                for t in range(2):
                    lanes = slice(128 * t, 128 * t + 128)
                    d_ref[row + r, subs, lanes] = src_ref[16 + r, subs, lanes] * mul + add
                d_ref[row + r, subs, COLS:] = spread(de, dw, g) * mul + add


def split_kron(kron_ref):
    kron = kron_ref[...]
    hi = kron.astype(jnp.bfloat16)
    return hi, (kron - hi.astype(F32)).astype(jnp.bfloat16)


def run_blocks(blocks, p_refs, d_ref, coef_ref, kron, mix_refs):
    kron_hi, kron_lo = kron

    def mix(index):
        step, r0 = blocks[index]
        flat = p_refs[step - 1][r0 : r0 + 8].reshape(8 * CH, EXT_COLS)
        hi = flat.astype(jnp.bfloat16)
        lo = (flat - hi.astype(F32)).astype(jnp.bfloat16)
        mixed = jnp.dot(kron_hi, hi, preferred_element_type=F32)
        mixed = mixed + jnp.dot(kron_hi, lo, preferred_element_type=F32)
        mixed = mixed + jnp.dot(kron_lo, hi, preferred_element_type=F32)
        mix_refs[index % 2][...] = mixed.reshape(8, CH, EXT_COLS)

    mix(0)
    for index, (step, r0) in enumerate(blocks):
        more = index + 1 < len(blocks)
        late = more and blocks[index + 1][0] == step + 1 and abs(blocks[index + 1][1] - r0) < 8
        if more and not late:
            mix(index + 1)
        src, dst = p_refs[step - 1], p_refs[step]
        for i in range(8):
            r = r0 + i
            c = src[r]
            acc = mix_refs[index % 2][i] + d_ref[r] * c
            if step > 1:
                acc = acc - p_refs[step - 2][r]
            coef = [coef_ref[k, r : r + 1] for k in range(6)]
            acc = acc + coef[0] * pltpu.roll(c, EXT_COLS - 1, 1)
            acc = acc + coef[1] * pltpu.roll(c, 1, 1)
            acc = acc + coef[2] * (pltpu.roll(c, EXT_COLS - 2, 1) - pltpu.roll(c, 2, 1))
            acc = acc + coef[3] * src[r + 1]
            acc = acc + coef[4] * src[r - 1]
            acc = acc + coef[5] * (src[r + 2] - src[r - 2])
            dst[r] = acc
        if late:
            mix(index + 1)


def cover(low, high):
    return [min(r, high - 8) for r in range(low, high, 8)]


INNER_STEPS = 6
INNER = [(j, r) for j in range(1, INNER_STEPS + 1) for r in cover(RIM + 2 * j, RIM + ROWS - 2 * j)]
OUTER = [
    (j, r)
    for j in range(1, NUM)
    for r in (
        cover(2 * j, RIM + 2 * j) + cover(RIM + ROWS - 2 * j, EXT_ROWS - 2 * j)
        if j <= INNER_STEPS
        else cover(2 * j, EXT_ROWS - 2 * j)
    )
]


def inner_kernel(s1_ref, s2_ref, g1_ref, g2_ref, tab_ref, kron_ref, *refs):
    p_refs = refs[: INNER_STEPS + 1]
    d_ref, coef_ref, k_ref = refs[INNER_STEPS + 1 : INNER_STEPS + 4]
    mix_refs, sem = refs[INNER_STEPS + 4 : INNER_STEPS + 6], refs[-1]
    start = pl.multiple_of(lax.axis_index("gy") * ROWS, ROWS)
    copy = pltpu.make_async_copy(tab_ref.at[pl.ds(start, EXT_ROWS)], k_ref, sem)
    copy.start()
    par_y = lax.rem(lax.axis_index("gy"), 2)
    kron = split_kron(kron_ref)
    copy.wait()
    for src_ref, half in ((s1_ref, 1 - par_y), (s2_ref, par_y)):
        place_half(
            src_ref, lambda sl, h=half: g1_ref[h, sl], lambda sl, h=half: g2_ref[h, sl],
            RIM + 16 * half, half, p_refs[0], d_ref, coef_ref, k_ref,
        )
    run_blocks(INNER, p_refs, d_ref, coef_ref, kron, mix_refs)


def outer_kernel(r1_ref, r2_ref, c1_ref, c2_ref, k_ref, kron_ref, *refs):
    refs = refs[INNER_STEPS + 3 :]
    p_refs = refs[: INNER_STEPS + 1] + refs[INNER_STEPS + 3 : NUM + 2]
    d_ref, coef_ref = refs[INNER_STEPS + 1 : INNER_STEPS + 3]
    gram_ref, mix_a, mix_b, sums_ref = refs[NUM + 2 :]
    par_y = lax.rem(lax.axis_index("gy"), 2)
    kron = split_kron(kron_ref)
    for src_ref, c_ref, row, half in (
        (r1_ref, c1_ref, 48 - 48 * par_y, par_y),
        (r2_ref, c2_ref, 48 * par_y, 1 - par_y),
    ):
        place_half(
            src_ref, lambda sl, c=c_ref: c[0, sl], lambda sl, c=c_ref: c[1, sl],
            row, half, p_refs[0], d_ref, coef_ref, k_ref,
        )
    run_blocks(OUTER, p_refs, d_ref, coef_ref, kron, (mix_a, mix_b))

    sums_ref[...] = jnp.zeros_like(sums_ref)
    for lo_k, hi_k in ((0, 6), (6, NUM)):
        pairs = [(n, i, j) for n, (i, j) in enumerate(PAIRS) if lo_k <= j < hi_k]

        def body(r, accs, pairs=pairs, hi_k=hi_k):
            accs = list(accs)
            for u in range(2):
                for c in range(2):
                    for t in range(2):
                        vecs = [
                            p_refs[k][RIM + 2 * r + u, 8 * c : 8 * c + 8, 128 * t : 128 * t + 128]
                            for k in range(hi_k)
                        ]
                        for n, (_, i, j) in enumerate(pairs):
                            accs[n] = accs[n] + vecs[i] * vecs[j]
            return tuple(accs)

        accs = lax.fori_loop(0, ROWS // 2, body, tuple(jnp.zeros((8, 128), F32) for _ in pairs))
        for (n, _, _), acc in zip(pairs, accs):
            sums_ref[n : n + 1, :] = jnp.sum(acc, axis=0, keepdims=True)
    gram_ref[...] = lax.dot_general(
        jnp.ones((128, 128), F32), sums_ref[...], (((1,), (1,)), ((), ())),
        precision=lax.Precision.HIGHEST, preferred_element_type=F32,
    )


def small_solve(gram):
    inv = 1.0 / SCALE

    def total(values):
        values = list(values)
        while len(values) > 1:
            nxt = [values[k] + values[k + 1] for k in range(0, len(values) - 1, 2)]
            if len(values) % 2:
                nxt.append(values[-1])
            values = nxt
        return values[0]

    def shifted(vec):
        out = []
        for k in range(len(vec) + 1):
            terms = [vec[m] for m in (k - 1, k + 1) if 0 <= m < len(vec)]
            parts = [total(terms) * inv] if terms else []
            if k < len(vec):
                parts.append(vec[k] * CENTRE)
            out.append(total(parts))
        return out

    def dot(one, two):
        return total(x * y for x, y in zip(one, two))

    first = jnp.sqrt(gram[0][0] + GUARD)
    inv_first = 1.0 / first
    basis = [[inv_first]]
    images = [[gram[k][0] * inv_first for k in range(NUM)]]
    cosines, sines, upper = [], [], []
    target = [first]
    for col in range(ITERS):
        work = shifted(basis[col])
        image = [dot(work, gram[k]) for k in range(NUM)]
        coeffs = [dot(basis[i], image) for i in range(col + 1)]
        work = [
            total([work[k]] + [-(coeffs[i] * basis[i][k]) for i in range(col + 1) if k < len(basis[i])])
            for k in range(len(work))
        ]
        image = [total([image[k]] + [-(coeffs[i] * images[i][k]) for i in range(col + 1)]) for k in range(NUM)]
        subdiag = jnp.sqrt(jnp.maximum(dot(work, image), 0.0) + GUARD)
        if col + 1 < ITERS:
            scale = 1.0 / subdiag
            basis.append([x * scale for x in work])
            images.append([x * scale for x in image])
        column = list(coeffs)
        for k in range(col):
            a, b = column[k], column[k + 1]
            column[k] = cosines[k] * a + sines[k] * b
            column[k + 1] = cosines[k] * b - sines[k] * a
        a, b = column[col], subdiag
        radius = jnp.sqrt(a * a + b * b)
        inv_radius = 1.0 / radius
        cosines.append(a * inv_radius)
        sines.append(b * inv_radius)
        column[col] = radius
        upper.append((column, inv_radius))
        last = target[col]
        target[col] = cosines[col] * last
        target.append(-(sines[col] * last))
    weights = [None] * ITERS
    for col in reversed(range(ITERS)):
        rest = [target[col]] + [-(upper[k][0][col] * weights[k]) for k in range(col + 1, ITERS)]
        weights[col] = total(rest) * upper[col][1]
    coef = [total([weights[j] * basis[j][k] for j in range(k, ITERS)]) for k in range(ITERS)]
    return coef, shifted(coef)


def final_kernel(*refs):
    p_refs = refs[:NUM]
    rows_ref, x_ref, r_ref, xv_ref, rv_ref, work_ref, sem = refs[NUM:]
    summed = jnp.sum(rows_ref[...], axis=0, keepdims=True)
    gram = [[None] * NUM for _ in range(NUM)]
    for n, (i, j) in enumerate(PAIRS):
        gram[i][j] = gram[j][i] = jnp.broadcast_to(summed[:, n : n + 1], (8, 128))
    coef, image = small_solve(gram)
    for k in range(ITERS):
        work_ref[k] = coef[k]
    work_ref[ITERS] = 1.0 - image[0]
    for k in range(1, NUM):
        work_ref[ITERS + k] = -image[k]
    copies = []
    for b in range(ROWS // 8):
        rows = slice(8 * b, 8 * b + 8)
        for c in range(2):
            for t in range(2):
                xs = rs = None
                for k in range(NUM):
                    vec = p_refs[k][RIM + 8 * b : RIM + 8 * b + 8, 8 * c : 8 * c + 8, 128 * t : 128 * t + 128]
                    part = vec * work_ref[ITERS + k]
                    rs = part if rs is None else rs + part
                    if k < ITERS:
                        part = vec * work_ref[k]
                        xs = part if xs is None else xs + part
                where = (slice(8 * c, 8 * c + 8), rows, slice(128 * t, 128 * t + 128))
                xv_ref[where] = jnp.swapaxes(xs, 0, 1)
                rv_ref[where] = jnp.swapaxes(rs, 0, 1)
        for n, (src, dst) in enumerate(((xv_ref, x_ref), (rv_ref, r_ref))):
            copy = pltpu.make_async_copy(src.at[:, rows], dst.at[:, rows], sem.at[2 * b + n])
            copy.start()
            copies.append(copy)
    for copy in copies:
        copy.wait()


def diffusion_table(lat_total):
    row = np.arange(-RIM, lat_total + RIM, dtype=np.float64)
    phi = -math.pi / 2 + (row + 0.5) * (math.pi / lat_total)
    kx = DIFF_LON / (np.cos(phi) ** 2 + 0.1)
    kx = np.where((row >= 0) & (row < lat_total), kx, 0.0)
    return np.repeat(kx[:, None], 128, axis=1).astype(np.float32)


VMEM = pl.BlockSpec(memory_space=pltpu.VMEM)
HBM = pl.BlockSpec(memory_space=pltpu.HBM)


def shape(*dims):
    return jax.ShapeDtypeStruct(dims, F32)


def pairing(count, odd, closed):
    pairs = []
    for i in range(count):
        partner = i + 1 if (i % 2 == 0) != odd else i - 1
        if closed:
            partner %= count
        if 0 <= partner < count:
            pairs.append((i, partner))
    return pairs


def per_device(forcing, damping, coupling, wind_lon, wind_lat, *, nx, ny):
    s1, s2, x1, x2 = pl.pallas_call(
        pack_kernel,
        in_specs=[VMEM] * 4,
        out_specs=[VMEM] * 4,
        out_shape=[shape(34, 16, COLS)] * 2 + [shape(2, 72, 128)] * 2,
        compiler_params=pltpu.CompilerParams(vmem_limit_bytes=8 * 2**20),
        name="pack",
    )(forcing, damping, wind_lon, wind_lat)
    g1 = lax.ppermute(x1, "gx", pairing(nx, False, True))
    g2 = lax.ppermute(x2, "gx", pairing(nx, True, True))
    r1 = lax.ppermute(s1, "gy", pairing(ny, False, False))
    r2 = lax.ppermute(s2, "gy", pairing(ny, True, False))
    both = jnp.stack([g1, g2])
    par_y = lax.rem(lax.axis_index("gy"), 2)
    k1 = lax.dynamic_index_in_dim(both, 1 - par_y, 1, keepdims=False)
    k2 = lax.dynamic_index_in_dim(both, par_y, 1, keepdims=False)
    c1 = lax.ppermute(k1, "gy", pairing(ny, False, False))
    c2 = lax.ppermute(k2, "gy", pairing(ny, True, False))
    table = jnp.asarray(diffusion_table(ny * ROWS))
    kron = jnp.kron(jnp.eye(8, dtype=F32), coupling * (COUPLE * SCALE))
    field = shape(EXT_ROWS, CH, EXT_COLS)
    mix = [pltpu.VMEM((8, CH, EXT_COLS), F32)] * 2
    carried = [field] * (INNER_STEPS + 2) + [shape(6, EXT_ROWS, EXT_COLS)]
    *state, k_rows = pl.pallas_call(
        inner_kernel,
        in_specs=[VMEM] * 4 + [HBM, VMEM],
        out_specs=[VMEM] * (len(carried) + 1),
        out_shape=carried + [shape(EXT_ROWS, 128)],
        scratch_shapes=mix + [pltpu.SemaphoreType.DMA],
        compiler_params=pltpu.CompilerParams(vmem_limit_bytes=8 * 2**20),
        cost_estimate=pl.CostEstimate(flops=10**8, bytes_accessed=2**20, transcendentals=0),
        name="inner",
    )(s1, s2, g1, g2, table, kron)
    extra = [field] * (NUM - INNER_STEPS - 1)
    results = pl.pallas_call(
        outer_kernel,
        in_specs=[VMEM] * (6 + len(carried)),
        out_specs=[VMEM] * (len(carried) + len(extra) + 1),
        out_shape=carried + extra + [shape(128, 128)],
        input_output_aliases={6 + n: n for n in range(len(carried))},
        scratch_shapes=mix + [pltpu.VMEM((128, 128), F32)],
        compiler_params=pltpu.CompilerParams(vmem_limit_bytes=8 * 2**20),
        name="outer",
    )(r1, r2, c1, c2, k_rows, kron, *state)
    basis = results[: INNER_STEPS + 1] + results[len(carried) : -1]
    rows = lax.all_to_all(results[-1], ("gx", "gy"), 0, 0, tiled=True)
    return pl.pallas_call(
        final_kernel,
        in_specs=[VMEM] * (NUM + 1),
        out_specs=[HBM, HBM],
        out_shape=[shape(CH, ROWS, COLS)] * 2,
        scratch_shapes=[
            pltpu.VMEM((CH, ROWS, COLS), F32),
            pltpu.VMEM((CH, ROWS, COLS), F32),
            pltpu.VMEM((ITERS + NUM, 8, 128), F32),
            pltpu.SemaphoreType.DMA((ROWS // 4,)),
        ],
        compiler_params=pltpu.CompilerParams(vmem_limit_bytes=8 * 2**20),
        name="finish",
    )(*basis, rows)


def solution(mesh):
    spec = P(None, "gy", "gx")
    flat = P("gy", "gx")
    return jax.shard_map(
        functools.partial(per_device, nx=mesh.shape["gx"], ny=mesh.shape["gy"]),
        mesh=mesh,
        in_specs=(spec, spec, P(), flat, flat),
        out_specs=(spec, spec),
        check_vma=False,
    )
```

```python
import functools
import math

import jax
import jax.numpy as jnp
import numpy as np
from jax import lax
from jax.experimental import pallas as pl
from jax.experimental.pallas import tpu as pltpu
from jax.sharding import PartitionSpec as P


ITERS = 8
CH = 16
ROWS = 32
COLS = 256
RIM = 2 * ITERS
EXT_ROWS = ROWS + 2 * RIM
EXT_COLS = COLS + 128
COUPLE = 0.25
DIFF_LAT = 0.5
DIFF_LON = 0.5
GUARD = 1.0

LOW, HIGH = 1.5, 26.0
CENTRE = (LOW + HIGH) / 2
SCALE = 4.0 / (HIGH - LOW)
NUM = ITERS + 1
PAIRS = [(i, j) for j in range(NUM) for i in range(j + 1)]
F32 = jnp.float32


def pack_kernel(
    f_hbm, d_hbm, wl_hbm, wt_hbm, s1_ref, s2_ref, x1_ref, x2_ref, f_ref, d_ref, wl_ref, wt_ref, sem
):
    copies = [
        pltpu.make_async_copy(src, dst, sem.at[n])
        for n, (src, dst) in enumerate(
            ((f_hbm, f_ref), (d_hbm, d_ref), (wl_hbm, wl_ref), (wt_hbm, wt_ref))
        )
    ]
    for copy in copies:
        copy.start()
    for copy in copies:
        copy.wait()
    par_y = lax.rem(lax.axis_index("gy"), 2)
    par_x = lax.rem(lax.axis_index("gx"), 2)
    for ref, half in ((s1_ref, 1 - par_y), (s2_ref, par_y)):
        for q in range(2):
            off = pl.multiple_of(half * 16 + 8 * q, 8)
            for src, base in ((f_ref, 0), (d_ref, 16)):
                for c in range(2):
                    ref[base + 8 * q : base + 8 * q + 8, 8 * c : 8 * c + 8, :] = jnp.swapaxes(
                        src[8 * c : 8 * c + 8, pl.ds(off, 8), :], 0, 1
                    )
        off = pl.multiple_of(half * 16, 16)
        ref[32] = wl_ref[pl.ds(off, 16), :]
        ref[33] = wt_ref[pl.ds(off, 16), :]
    group = lax.broadcasted_iota(jnp.int32, (8, 128), 1) // 16

    def gather(tiles):
        left = jnp.zeros((8, 128), F32)
        right = jnp.zeros((8, 128), F32)
        for g, (low, high) in enumerate(tiles):
            left = jnp.where(group == g, pltpu.roll(low, 16 * g, 1) if g else low, left)
            shift = (16 * g + 16) % 128
            right = jnp.where(group == g, pltpu.roll(high, shift, 1) if shift else high, right)
        return jnp.where(par_x == 0, right, left), jnp.where(par_x == 0, left, right)

    winds = gather(
        [
            (ref[8 * q : 8 * q + 8, :128], ref[8 * q : 8 * q + 8, 128:])
            for ref in (wl_ref, wt_ref)
            for q in range(4)
        ]
    )
    for half in range(2):
        slot = 0
        for base in (0, 16):
            for q in range(2):
                for c in range(2):
                    tiles = []
                    for g in range(8):
                        row = base + 8 * q + g
                        pick = []
                        for t in range(2):
                            one = s1_ref[row, 8 * c : 8 * c + 8, 128 * t : 128 * t + 128]
                            two = s2_ref[row, 8 * c : 8 * c + 8, 128 * t : 128 * t + 128]
                            pick.append(jnp.where(par_y == half, two, one))
                        tiles.append(tuple(pick))
                    first, second = gather(tiles)
                    x1_ref[half, 8 * slot : 8 * slot + 8, :] = first
                    x2_ref[half, 8 * slot : 8 * slot + 8, :] = second
                    slot += 1
        x1_ref[half, 64:72, :] = winds[0]
        x2_ref[half, 64:72, :] = winds[1]


LANE_SHAPE = (8, 128)


def place_half(src_ref, one, two, row, half, p0_ref, d_ref, coef_ref, k_ref):
    par_x = lax.rem(lax.axis_index("gx"), 2)
    lane = lax.broadcasted_iota(jnp.int32, LANE_SHAPE, 1)
    row = pl.multiple_of(row, 16)

    def spread(east, west, g):
        e = pltpu.roll(east, (128 - 16 * g) % 128, 1) if g else east
        shift = (112 - 16 * g) % 128
        w = pltpu.roll(west, shift, 1) if shift else west
        return jnp.where(lane < 16, e, jnp.where(lane >= 112, w, 0.0))

    def sides(slot):
        a = one(slice(8 * slot, 8 * slot + 8))
        b = two(slice(8 * slot, 8 * slot + 8))
        return jnp.where(par_x == 0, a, b), jnp.where(par_x == 0, b, a)

    east, west = sides(8)
    scales = []
    for q in range(2):
        rows = pl.ds(pl.multiple_of(row + 8 * q, 8), 8)
        k = k_ref[rows]
        live = jnp.where(k > 0.0, 1.0, 0.0)
        kx = k * SCALE
        half_lat = live * (SCALE * DIFF_LAT)
        fixed = live * (SCALE * (1.0 + 2.0 * DIFF_LAT - CENTRE)) + 2.0 * kx
        for t in range(3):
            lanes = slice(128 * t, 128 * t + 128)
            winds = []
            for field in range(2):
                if t < 2:
                    wind = src_ref[32 + field, 8 * q : 8 * q + 8, lanes]
                else:
                    low = spread(east, west, 4 * field + q)
                    high = spread(east, west, 4 * field + 2 + q)
                    wind = jnp.where(half == 0, low, high)
                winds.append(wind * (live * (SCALE / 12.0)))
            lon, lat = winds
            coef_ref[0, rows, lanes] = 8.0 * lon - kx
            coef_ref[1, rows, lanes] = -8.0 * lon - kx
            coef_ref[2, rows, lanes] = -lon
            coef_ref[3, rows, lanes] = 8.0 * lat - half_lat
            coef_ref[4, rows, lanes] = -8.0 * lat - half_lat
            coef_ref[5, rows, lanes] = -lat
        scales.append((live * SCALE, fixed))
    for q in range(2):
        for c in range(2):
            subs = slice(8 * c, 8 * c + 8)
            fe, fw = sides(2 * q + c)
            de, dw = sides(4 + 2 * q + c)
            for g in range(8):
                r = 8 * q + g
                p0_ref[row + r, subs, :COLS] = src_ref[r, subs]
                p0_ref[row + r, subs, COLS:] = spread(fe, fw, g)
                mul, add = (x[g : g + 1] for x in scales[q])
                for t in range(2):
                    lanes = slice(128 * t, 128 * t + 128)
                    d_ref[row + r, subs, lanes] = src_ref[16 + r, subs, lanes] * mul + add
                d_ref[row + r, subs, COLS:] = spread(de, dw, g) * mul + add


def split_kron(kron_ref):
    kron = kron_ref[...]
    hi = kron.astype(jnp.bfloat16)
    return hi, (kron - hi.astype(F32)).astype(jnp.bfloat16)


def run_blocks(blocks, p_refs, d_ref, coef_ref, kron, mix_refs):
    kron_hi, kron_lo = kron

    def mix(index):
        step, r0 = blocks[index]
        flat = p_refs[step - 1][r0 : r0 + 8].reshape(8 * CH, EXT_COLS)
        hi = flat.astype(jnp.bfloat16)
        lo = (flat - hi.astype(F32)).astype(jnp.bfloat16)
        mixed = jnp.dot(kron_hi, hi, preferred_element_type=F32)
        mixed = mixed + jnp.dot(kron_hi, lo, preferred_element_type=F32)
        mixed = mixed + jnp.dot(kron_lo, hi, preferred_element_type=F32)
        mix_refs[index % 2][...] = mixed.reshape(8, CH, EXT_COLS)

    mix(0)
    for index, (step, r0) in enumerate(blocks):
        more = index + 1 < len(blocks)
        late = more and blocks[index + 1][0] == step + 1 and abs(blocks[index + 1][1] - r0) < 8
        if more and not late:
            mix(index + 1)
        src, dst = p_refs[step - 1], p_refs[step]
        for i in range(8):
            r = r0 + i
            c = src[r]
            acc = mix_refs[index % 2][i] + d_ref[r] * c
            if step > 1:
                acc = acc - p_refs[step - 2][r]
            coef = [coef_ref[k, r : r + 1] for k in range(6)]
            acc = acc + coef[0] * pltpu.roll(c, EXT_COLS - 1, 1)
            acc = acc + coef[1] * pltpu.roll(c, 1, 1)
            acc = acc + coef[2] * (pltpu.roll(c, EXT_COLS - 2, 1) - pltpu.roll(c, 2, 1))
            acc = acc + coef[3] * src[r + 1]
            acc = acc + coef[4] * src[r - 1]
            acc = acc + coef[5] * (src[r + 2] - src[r - 2])
            dst[r] = acc
        if late:
            mix(index + 1)


def cover(low, high):
    return [min(r, high - 8) for r in range(low, high, 8)]


INNER_STEPS = 6
INNER = [(j, r) for j in range(1, INNER_STEPS + 1) for r in cover(RIM + 2 * j, RIM + ROWS - 2 * j)]
OUTER = [
    (j, r)
    for j in range(1, NUM)
    for r in (
        cover(2 * j, RIM + 2 * j) + cover(RIM + ROWS - 2 * j, EXT_ROWS - 2 * j)
        if j <= INNER_STEPS
        else cover(2 * j, EXT_ROWS - 2 * j)
    )
]


def inner_kernel(s1_ref, s2_ref, g1_ref, g2_ref, tab_ref, kron_ref, *refs):
    p_refs = refs[: INNER_STEPS + 1]
    d_ref, coef_ref, k_ref = refs[INNER_STEPS + 1 : INNER_STEPS + 4]
    mix_refs, sem = refs[INNER_STEPS + 4 : INNER_STEPS + 6], refs[-1]
    start = pl.multiple_of(lax.axis_index("gy") * ROWS, ROWS)
    copy = pltpu.make_async_copy(tab_ref.at[pl.ds(start, EXT_ROWS)], k_ref, sem)
    copy.start()
    par_y = lax.rem(lax.axis_index("gy"), 2)
    kron = split_kron(kron_ref)
    copy.wait()
    for src_ref, half in ((s1_ref, 1 - par_y), (s2_ref, par_y)):
        place_half(
            src_ref, lambda sl, h=half: g1_ref[h, sl], lambda sl, h=half: g2_ref[h, sl],
            RIM + 16 * half, half, p_refs[0], d_ref, coef_ref, k_ref,
        )
    run_blocks(INNER, p_refs, d_ref, coef_ref, kron, mix_refs)


def outer_kernel(r1_ref, r2_ref, c1_ref, c2_ref, k_ref, kron_ref, *refs):
    refs = refs[INNER_STEPS + 3 :]
    p_refs = refs[: INNER_STEPS + 1] + refs[INNER_STEPS + 3 : NUM + 2]
    d_ref, coef_ref = refs[INNER_STEPS + 1 : INNER_STEPS + 3]
    gram_ref, mix_a, mix_b, sums_ref = refs[NUM + 2 :]
    par_y = lax.rem(lax.axis_index("gy"), 2)
    kron = split_kron(kron_ref)
    for src_ref, c_ref, row, half in (
        (r1_ref, c1_ref, 48 - 48 * par_y, par_y),
        (r2_ref, c2_ref, 48 * par_y, 1 - par_y),
    ):
        place_half(
            src_ref, lambda sl, c=c_ref: c[0, sl], lambda sl, c=c_ref: c[1, sl],
            row, half, p_refs[0], d_ref, coef_ref, k_ref,
        )
    run_blocks(OUTER, p_refs, d_ref, coef_ref, kron, (mix_a, mix_b))

    sums_ref[...] = jnp.zeros_like(sums_ref)
    for lo_k, hi_k in ((0, 6), (6, NUM)):
        pairs = [(n, i, j) for n, (i, j) in enumerate(PAIRS) if lo_k <= j < hi_k]

        def body(r, accs, pairs=pairs, hi_k=hi_k):
            accs = list(accs)
            for u in range(2):
                for c in range(2):
                    for t in range(2):
                        vecs = [
                            p_refs[k][RIM + 2 * r + u, 8 * c : 8 * c + 8, 128 * t : 128 * t + 128]
                            for k in range(hi_k)
                        ]
                        for n, (_, i, j) in enumerate(pairs):
                            accs[n] = accs[n] + vecs[i] * vecs[j]
            return tuple(accs)

        accs = lax.fori_loop(0, ROWS // 2, body, tuple(jnp.zeros((8, 128), F32) for _ in pairs))
        for (n, _, _), acc in zip(pairs, accs):
            sums_ref[n : n + 1, :] = jnp.sum(acc, axis=0, keepdims=True)
    gram_ref[...] = lax.dot_general(
        jnp.ones((128, 128), F32), sums_ref[...], (((1,), (1,)), ((), ())),
        precision=lax.Precision.HIGHEST, preferred_element_type=F32,
    )


def small_solve(gram):
    inv = 1.0 / SCALE

    def total(values):
        values = list(values)
        while len(values) > 1:
            nxt = [values[k] + values[k + 1] for k in range(0, len(values) - 1, 2)]
            if len(values) % 2:
                nxt.append(values[-1])
            values = nxt
        return values[0]

    def shifted(vec):
        out = []
        for k in range(len(vec) + 1):
            terms = [vec[m] for m in (k - 1, k + 1) if 0 <= m < len(vec)]
            parts = [total(terms) * inv] if terms else []
            if k < len(vec):
                parts.append(vec[k] * CENTRE)
            out.append(total(parts))
        return out

    def dot(one, two):
        return total(x * y for x, y in zip(one, two))

    first = jnp.sqrt(gram[0][0] + GUARD)
    inv_first = 1.0 / first
    basis = [[inv_first]]
    images = [[gram[k][0] * inv_first for k in range(NUM)]]
    cosines, sines, upper = [], [], []
    target = [first]
    for col in range(ITERS):
        work = shifted(basis[col])
        image = [dot(work, gram[k]) for k in range(NUM)]
        coeffs = [dot(basis[i], image) for i in range(col + 1)]
        work = [
            total([work[k]] + [-(coeffs[i] * basis[i][k]) for i in range(col + 1) if k < len(basis[i])])
            for k in range(len(work))
        ]
        image = [total([image[k]] + [-(coeffs[i] * images[i][k]) for i in range(col + 1)]) for k in range(NUM)]
        subdiag = jnp.sqrt(jnp.maximum(dot(work, image), 0.0) + GUARD)
        if col + 1 < ITERS:
            scale = 1.0 / subdiag
            basis.append([x * scale for x in work])
            images.append([x * scale for x in image])
        column = list(coeffs)
        for k in range(col):
            a, b = column[k], column[k + 1]
            column[k] = cosines[k] * a + sines[k] * b
            column[k + 1] = cosines[k] * b - sines[k] * a
        a, b = column[col], subdiag
        radius = jnp.sqrt(a * a + b * b)
        inv_radius = 1.0 / radius
        cosines.append(a * inv_radius)
        sines.append(b * inv_radius)
        column[col] = radius
        upper.append((column, inv_radius))
        last = target[col]
        target[col] = cosines[col] * last
        target.append(-(sines[col] * last))
    weights = [None] * ITERS
    for col in reversed(range(ITERS)):
        rest = [target[col]] + [-(upper[k][0][col] * weights[k]) for k in range(col + 1, ITERS)]
        weights[col] = total(rest) * upper[col][1]
    coef = [total([weights[j] * basis[j][k] for j in range(k, ITERS)]) for k in range(ITERS)]
    return coef, shifted(coef)


def final_kernel(*refs):
    p_refs = refs[:NUM]
    rows_ref, x_ref, r_ref, xv_ref, rv_ref, work_ref, sem = refs[NUM:]
    summed = jnp.sum(rows_ref[...], axis=0, keepdims=True)
    gram = [[None] * NUM for _ in range(NUM)]
    for n, (i, j) in enumerate(PAIRS):
        gram[i][j] = gram[j][i] = jnp.broadcast_to(summed[:, n : n + 1], (8, 128))
    coef, image = small_solve(gram)
    for k in range(ITERS):
        work_ref[k] = coef[k]
    work_ref[ITERS] = 1.0 - image[0]
    for k in range(1, NUM):
        work_ref[ITERS + k] = -image[k]
    copies = []
    for b in range(ROWS // 8):
        rows = slice(8 * b, 8 * b + 8)
        for c in range(2):
            for t in range(2):
                xs = rs = None
                for k in range(NUM):
                    vec = p_refs[k][RIM + 8 * b : RIM + 8 * b + 8, 8 * c : 8 * c + 8, 128 * t : 128 * t + 128]
                    part = vec * work_ref[ITERS + k]
                    rs = part if rs is None else rs + part
                    if k < ITERS:
                        part = vec * work_ref[k]
                        xs = part if xs is None else xs + part
                where = (slice(8 * c, 8 * c + 8), rows, slice(128 * t, 128 * t + 128))
                xv_ref[where] = jnp.swapaxes(xs, 0, 1)
                rv_ref[where] = jnp.swapaxes(rs, 0, 1)
        for n, (src, dst) in enumerate(((xv_ref, x_ref), (rv_ref, r_ref))):
            copy = pltpu.make_async_copy(src.at[:, rows], dst.at[:, rows], sem.at[2 * b + n])
            copy.start()
            copies.append(copy)
    for copy in copies:
        copy.wait()


def diffusion_table(lat_total):
    row = np.arange(-RIM, lat_total + RIM, dtype=np.float64)
    phi = -math.pi / 2 + (row + 0.5) * (math.pi / lat_total)
    kx = DIFF_LON / (np.cos(phi) ** 2 + 0.1)
    kx = np.where((row >= 0) & (row < lat_total), kx, 0.0)
    return np.repeat(kx[:, None], 128, axis=1).astype(np.float32)


VMEM = pl.BlockSpec(memory_space=pltpu.VMEM)
HBM = pl.BlockSpec(memory_space=pltpu.HBM)


def shape(*dims):
    return jax.ShapeDtypeStruct(dims, F32)


def pairing(count, odd, closed):
    pairs = []
    for i in range(count):
        partner = i + 1 if (i % 2 == 0) != odd else i - 1
        if closed:
            partner %= count
        if 0 <= partner < count:
            pairs.append((i, partner))
    return pairs


def per_device(forcing, damping, coupling, wind_lon, wind_lat, *, nx, ny):
    s1, s2, x1, x2 = pl.pallas_call(
        pack_kernel,
        in_specs=[HBM] * 4,
        out_specs=[VMEM] * 4,
        out_shape=[shape(34, 16, COLS)] * 2 + [shape(2, 72, 128)] * 2,
        scratch_shapes=[
            pltpu.VMEM((CH, ROWS, COLS), F32),
            pltpu.VMEM((CH, ROWS, COLS), F32),
            pltpu.VMEM((ROWS, COLS), F32),
            pltpu.VMEM((ROWS, COLS), F32),
            pltpu.SemaphoreType.DMA((4,)),
        ],
        compiler_params=pltpu.CompilerParams(vmem_limit_bytes=8 * 2**20),
        name="pack",
    )(*(pltpu.with_memory_space_constraint(x, pltpu.HBM) for x in (forcing, damping, wind_lon, wind_lat)))
    r1 = lax.ppermute(s1, "gy", pairing(ny, False, False))
    r2 = lax.ppermute(s2, "gy", pairing(ny, True, False))
    g1 = lax.ppermute(x1, "gx", pairing(nx, False, True))
    g2 = lax.ppermute(x2, "gx", pairing(nx, True, True))
    both = jnp.stack([g1, g2])
    par_y = lax.rem(lax.axis_index("gy"), 2)
    k1 = lax.dynamic_index_in_dim(both, 1 - par_y, 1, keepdims=False)
    k2 = lax.dynamic_index_in_dim(both, par_y, 1, keepdims=False)
    c1 = lax.ppermute(k1, "gy", pairing(ny, False, False))
    c2 = lax.ppermute(k2, "gy", pairing(ny, True, False))
    table = jnp.asarray(diffusion_table(ny * ROWS))
    kron = jnp.kron(jnp.eye(8, dtype=F32), coupling * (COUPLE * SCALE))
    field = shape(EXT_ROWS, CH, EXT_COLS)
    mix = [pltpu.VMEM((8, CH, EXT_COLS), F32)] * 2
    carried = [field] * (INNER_STEPS + 2) + [shape(6, EXT_ROWS, EXT_COLS)]
    *state, k_rows = pl.pallas_call(
        inner_kernel,
        in_specs=[VMEM] * 4 + [HBM, VMEM],
        out_specs=[VMEM] * (len(carried) + 1),
        out_shape=carried + [shape(EXT_ROWS, 128)],
        scratch_shapes=mix + [pltpu.SemaphoreType.DMA],
        compiler_params=pltpu.CompilerParams(vmem_limit_bytes=8 * 2**20),
        cost_estimate=pl.CostEstimate(flops=10**8, bytes_accessed=2**20, transcendentals=0),
        name="inner",
    )(s1, s2, g1, g2, table, kron)
    extra = [field] * (NUM - INNER_STEPS - 1)
    results = pl.pallas_call(
        outer_kernel,
        in_specs=[VMEM] * (6 + len(carried)),
        out_specs=[VMEM] * (len(carried) + len(extra) + 1),
        out_shape=carried + extra + [shape(128, 128)],
        input_output_aliases={6 + n: n for n in range(len(carried))},
        scratch_shapes=mix + [pltpu.VMEM((128, 128), F32)],
        compiler_params=pltpu.CompilerParams(vmem_limit_bytes=8 * 2**20),
        name="outer",
    )(r1, r2, c1, c2, k_rows, kron, *state)
    basis = results[: INNER_STEPS + 1] + results[len(carried) : -1]
    rows = lax.all_to_all(results[-1], ("gx", "gy"), 0, 0, tiled=True)
    return pl.pallas_call(
        final_kernel,
        in_specs=[VMEM] * (NUM + 1),
        out_specs=[HBM, HBM],
        out_shape=[shape(CH, ROWS, COLS)] * 2,
        scratch_shapes=[
            pltpu.VMEM((CH, ROWS, COLS), F32),
            pltpu.VMEM((CH, ROWS, COLS), F32),
            pltpu.VMEM((ITERS + NUM, 8, 128), F32),
            pltpu.SemaphoreType.DMA((ROWS // 4,)),
        ],
        compiler_params=pltpu.CompilerParams(vmem_limit_bytes=8 * 2**20),
        name="finish",
    )(*basis, rows)


def solution(mesh):
    spec = P(None, "gy", "gx")
    flat = P("gy", "gx")
    return jax.shard_map(
        functools.partial(per_device, nx=mesh.shape["gx"], ny=mesh.shape["gy"]),
        mesh=mesh,
        in_specs=(spec, spec, P(), flat, flat),
        out_specs=(spec, spec),
        check_vma=False,
    )
```

```python
import functools
import math

import jax
import jax.numpy as jnp
import numpy as np
from jax import lax
from jax.experimental import pallas as pl
from jax.experimental.pallas import tpu as pltpu
from jax.sharding import PartitionSpec as P


ITERS = 8
CH = 16
ROWS = 32
COLS = 256
RIM = 2 * ITERS
EXT_ROWS = ROWS + 2 * RIM
EXT_COLS = COLS + 128
COUPLE = 0.25
DIFF_LAT = 0.5
DIFF_LON = 0.5
GUARD = 1.0

LOW, HIGH = 1.5, 26.0
CENTRE = (LOW + HIGH) / 2
SCALE = 4.0 / (HIGH - LOW)
NUM = ITERS + 1
PAIRS = [(i, j) for j in range(NUM) for i in range(j + 1)]
F32 = jnp.float32


def pack_kernel(
    f_hbm, d_hbm, wl_hbm, wt_hbm, cp_hbm, tab_hbm,
    s1_ref, s2_ref, x1_ref, x2_ref, cp_ref, k_ref,
    f_ref, d_ref, wl_ref, wt_ref, sem,
):
    start = pl.multiple_of(lax.axis_index("gy") * ROWS, ROWS)
    copies = [
        pltpu.make_async_copy(src, dst, sem.at[n])
        for n, (src, dst) in enumerate(
            (
                (f_hbm, f_ref), (d_hbm, d_ref), (wl_hbm, wl_ref), (wt_hbm, wt_ref),
                (cp_hbm, cp_ref), (tab_hbm.at[pl.ds(start, EXT_ROWS)], k_ref),
            )
        )
    ]
    for copy in copies:
        copy.start()
    for copy in copies:
        copy.wait()
    par_y = lax.rem(lax.axis_index("gy"), 2)
    par_x = lax.rem(lax.axis_index("gx"), 2)
    for ref, half in ((s1_ref, 1 - par_y), (s2_ref, par_y)):
        for q in range(2):
            off = pl.multiple_of(half * 16 + 8 * q, 8)
            for src, base in ((f_ref, 0), (d_ref, 16)):
                for c in range(2):
                    ref[base + 8 * q : base + 8 * q + 8, 8 * c : 8 * c + 8, :] = jnp.swapaxes(
                        src[8 * c : 8 * c + 8, pl.ds(off, 8), :], 0, 1
                    )
        off = pl.multiple_of(half * 16, 16)
        ref[32] = wl_ref[pl.ds(off, 16), :]
        ref[33] = wt_ref[pl.ds(off, 16), :]
    group = lax.broadcasted_iota(jnp.int32, (8, 128), 1) // 16

    def gather(tiles):
        left = jnp.zeros((8, 128), F32)
        right = jnp.zeros((8, 128), F32)
        for g, (low, high) in enumerate(tiles):
            left = jnp.where(group == g, pltpu.roll(low, 16 * g, 1) if g else low, left)
            shift = (16 * g + 16) % 128
            right = jnp.where(group == g, pltpu.roll(high, shift, 1) if shift else high, right)
        return jnp.where(par_x == 0, right, left), jnp.where(par_x == 0, left, right)

    winds = gather(
        [
            (ref[8 * q : 8 * q + 8, :128], ref[8 * q : 8 * q + 8, 128:])
            for ref in (wl_ref, wt_ref)
            for q in range(4)
        ]
    )
    for half in range(2):
        slot = 0
        for base in (0, 16):
            for q in range(2):
                for c in range(2):
                    tiles = []
                    for g in range(8):
                        row = base + 8 * q + g
                        pick = []
                        for t in range(2):
                            one = s1_ref[row, 8 * c : 8 * c + 8, 128 * t : 128 * t + 128]
                            two = s2_ref[row, 8 * c : 8 * c + 8, 128 * t : 128 * t + 128]
                            pick.append(jnp.where(par_y == half, two, one))
                        tiles.append(tuple(pick))
                    first, second = gather(tiles)
                    x1_ref[half, 8 * slot : 8 * slot + 8, :] = first
                    x2_ref[half, 8 * slot : 8 * slot + 8, :] = second
                    slot += 1
        x1_ref[half, 64:72, :] = winds[0]
        x2_ref[half, 64:72, :] = winds[1]


LANE_SHAPE = (8, 128)


def place_half(src_ref, one, two, row, half, p0_ref, d_ref, coef_ref, k_ref):
    par_x = lax.rem(lax.axis_index("gx"), 2)
    lane = lax.broadcasted_iota(jnp.int32, LANE_SHAPE, 1)
    row = pl.multiple_of(row, 16)

    def spread(east, west, g):
        e = pltpu.roll(east, (128 - 16 * g) % 128, 1) if g else east
        shift = (112 - 16 * g) % 128
        w = pltpu.roll(west, shift, 1) if shift else west
        return jnp.where(lane < 16, e, jnp.where(lane >= 112, w, 0.0))

    def sides(slot):
        a = one(slice(8 * slot, 8 * slot + 8))
        b = two(slice(8 * slot, 8 * slot + 8))
        return jnp.where(par_x == 0, a, b), jnp.where(par_x == 0, b, a)

    east, west = sides(8)
    scales = []
    for q in range(2):
        rows = pl.ds(pl.multiple_of(row + 8 * q, 8), 8)
        k = k_ref[rows]
        live = jnp.where(k > 0.0, 1.0, 0.0)
        kx = k * SCALE
        half_lat = live * (SCALE * DIFF_LAT)
        fixed = live * (SCALE * (1.0 + 2.0 * DIFF_LAT - CENTRE)) + 2.0 * kx
        for t in range(3):
            lanes = slice(128 * t, 128 * t + 128)
            winds = []
            for field in range(2):
                if t < 2:
                    wind = src_ref[32 + field, 8 * q : 8 * q + 8, lanes]
                else:
                    low = spread(east, west, 4 * field + q)
                    high = spread(east, west, 4 * field + 2 + q)
                    wind = jnp.where(half == 0, low, high)
                winds.append(wind * (live * (SCALE / 12.0)))
            lon, lat = winds
            coef_ref[0, rows, lanes] = 8.0 * lon - kx
            coef_ref[1, rows, lanes] = -8.0 * lon - kx
            coef_ref[2, rows, lanes] = -lon
            coef_ref[3, rows, lanes] = 8.0 * lat - half_lat
            coef_ref[4, rows, lanes] = -8.0 * lat - half_lat
            coef_ref[5, rows, lanes] = -lat
        scales.append((live * SCALE, fixed))
    for q in range(2):
        for c in range(2):
            subs = slice(8 * c, 8 * c + 8)
            fe, fw = sides(2 * q + c)
            de, dw = sides(4 + 2 * q + c)
            for g in range(8):
                r = 8 * q + g
                p0_ref[row + r, subs, :COLS] = src_ref[r, subs]
                p0_ref[row + r, subs, COLS:] = spread(fe, fw, g)
                mul, add = (x[g : g + 1] for x in scales[q])
                for t in range(2):
                    lanes = slice(128 * t, 128 * t + 128)
                    d_ref[row + r, subs, lanes] = src_ref[16 + r, subs, lanes] * mul + add
                d_ref[row + r, subs, COLS:] = spread(de, dw, g) * mul + add


def split_kron(kron_ref):
    kron = kron_ref[...]
    hi = kron.astype(jnp.bfloat16)
    return hi, (kron - hi.astype(F32)).astype(jnp.bfloat16)


def run_blocks(blocks, p_refs, d_ref, coef_ref, kron, mix_refs):
    kron_hi, kron_lo = kron

    def mix(index):
        step, r0 = blocks[index]
        flat = p_refs[step - 1][r0 : r0 + 8].reshape(8 * CH, EXT_COLS)
        hi = flat.astype(jnp.bfloat16)
        lo = (flat - hi.astype(F32)).astype(jnp.bfloat16)
        mixed = jnp.dot(kron_hi, hi, preferred_element_type=F32)
        mixed = mixed + jnp.dot(kron_hi, lo, preferred_element_type=F32)
        mixed = mixed + jnp.dot(kron_lo, hi, preferred_element_type=F32)
        mix_refs[index % 2][...] = mixed.reshape(8, CH, EXT_COLS)

    mix(0)
    for index, (step, r0) in enumerate(blocks):
        more = index + 1 < len(blocks)
        late = more and blocks[index + 1][0] == step + 1 and abs(blocks[index + 1][1] - r0) < 8
        if more and not late:
            mix(index + 1)
        src, dst = p_refs[step - 1], p_refs[step]
        for s in (slice(0, 8), slice(8, 16)):
            for i in range(8):
                r = r0 + i
                c = src[r, s]
                acc = mix_refs[index % 2][i, s] + d_ref[r, s] * c
                if step > 1:
                    acc = acc - p_refs[step - 2][r, s]
                coef = [coef_ref[k, r : r + 1] for k in range(6)]
                acc = acc + coef[0] * pltpu.roll(c, EXT_COLS - 1, 1)
                acc = acc + coef[1] * pltpu.roll(c, 1, 1)
                acc = acc + coef[2] * (pltpu.roll(c, EXT_COLS - 2, 1) - pltpu.roll(c, 2, 1))
                acc = acc + coef[3] * src[r + 1, s]
                acc = acc + coef[4] * src[r - 1, s]
                acc = acc + coef[5] * (src[r + 2, s] - src[r - 2, s])
                dst[r, s] = acc
        if late:
            mix(index + 1)


def cover(low, high):
    return [min(r, high - 8) for r in range(low, high, 8)]


INNER_STEPS = 6
INNER = [(j, r) for j in range(1, INNER_STEPS + 1) for r in cover(RIM + 2 * j, RIM + ROWS - 2 * j)]
OUTER = [
    (j, r)
    for j in range(1, NUM)
    for r in (
        cover(2 * j, RIM + 2 * j) + cover(RIM + ROWS - 2 * j, EXT_ROWS - 2 * j)
        if j <= INNER_STEPS
        else cover(2 * j, EXT_ROWS - 2 * j)
    )
]


def inner_kernel(s1_ref, s2_ref, g1_ref, g2_ref, cp_ref, k_ref, *refs):
    p_refs = refs[: INNER_STEPS + 1]
    d_ref, coef_ref, k1_ref, k2_ref, kron_ref, *mix_refs = refs[INNER_STEPS + 1 :]
    par_y = lax.rem(lax.axis_index("gy"), 2)
    for n, g_ref in enumerate((g1_ref, g2_ref)):
        k1_ref[n] = g_ref[1 - par_y]
        k2_ref[n] = g_ref[par_y]
    size = 8 * CH
    pick = lax.broadcasted_iota(jnp.int32, (size, CH), 0) % CH
    pick = (pick == lax.broadcasted_iota(jnp.int32, (size, CH), 1)).astype(F32)
    tall = jnp.dot(
        pick, cp_ref[...] * (COUPLE * SCALE), precision=lax.Precision.HIGHEST, preferred_element_type=F32
    )
    full = lax.dot_general(
        tall, pick, (((1,), (1,)), ((), ())), precision=lax.Precision.HIGHEST, preferred_element_type=F32
    )
    row = lax.broadcasted_iota(jnp.int32, (size, size), 0) // CH
    col = lax.broadcasted_iota(jnp.int32, (size, size), 1) // CH
    kron_ref[...] = jnp.where(row == col, full, 0.0)
    for src_ref, half in ((s1_ref, 1 - par_y), (s2_ref, par_y)):
        place_half(
            src_ref, lambda sl, h=half: g1_ref[h, sl], lambda sl, h=half: g2_ref[h, sl],
            RIM + 16 * half, half, p_refs[0], d_ref, coef_ref, k_ref,
        )
    run_blocks(INNER, p_refs, d_ref, coef_ref, split_kron(kron_ref), mix_refs)


def outer_kernel(r1_ref, r2_ref, c1_ref, c2_ref, k_ref, kron_ref, *refs):
    refs = refs[INNER_STEPS + 3 :]
    p_refs = refs[: INNER_STEPS + 1] + refs[INNER_STEPS + 3 : NUM + 2]
    d_ref, coef_ref = refs[INNER_STEPS + 1 : INNER_STEPS + 3]
    gram_ref, mix_a, mix_b, sums_ref = refs[NUM + 2 :]
    par_y = lax.rem(lax.axis_index("gy"), 2)
    kron = split_kron(kron_ref)
    for src_ref, c_ref, row, half in (
        (r1_ref, c1_ref, 48 - 48 * par_y, par_y),
        (r2_ref, c2_ref, 48 * par_y, 1 - par_y),
    ):
        place_half(
            src_ref, lambda sl, c=c_ref: c[0, sl], lambda sl, c=c_ref: c[1, sl],
            row, half, p_refs[0], d_ref, coef_ref, k_ref,
        )
    run_blocks(OUTER, p_refs, d_ref, coef_ref, kron, (mix_a, mix_b))

    sums_ref[...] = jnp.zeros_like(sums_ref)
    for lo_k, hi_k in ((0, 6), (6, NUM)):
        pairs = [(n, i, j) for n, (i, j) in enumerate(PAIRS) if lo_k <= j < hi_k]

        def body(r, accs, pairs=pairs, hi_k=hi_k):
            accs = list(accs)
            for u in range(2):
                for c in range(2):
                    for t in range(2):
                        vecs = [
                            p_refs[k][RIM + 2 * r + u, 8 * c : 8 * c + 8, 128 * t : 128 * t + 128]
                            for k in range(hi_k)
                        ]
                        for n, (_, i, j) in enumerate(pairs):
                            accs[n] = accs[n] + vecs[i] * vecs[j]
            return tuple(accs)

        accs = lax.fori_loop(0, ROWS // 2, body, tuple(jnp.zeros((8, 128), F32) for _ in pairs))
        for (n, _, _), acc in zip(pairs, accs):
            sums_ref[n : n + 1, :] = jnp.sum(acc, axis=0, keepdims=True)
    gram_ref[...] = lax.dot_general(
        jnp.ones((128, 128), F32), sums_ref[...], (((1,), (1,)), ((), ())),
        precision=lax.Precision.HIGHEST, preferred_element_type=F32,
    )


def small_solve(gram):
    inv = 1.0 / SCALE

    def total(values):
        values = list(values)
        while len(values) > 1:
            nxt = [values[k] + values[k + 1] for k in range(0, len(values) - 1, 2)]
            if len(values) % 2:
                nxt.append(values[-1])
            values = nxt
        return values[0]

    def shifted(vec):
        out = []
        for k in range(len(vec) + 1):
            terms = [vec[m] for m in (k - 1, k + 1) if 0 <= m < len(vec)]
            parts = [total(terms) * inv] if terms else []
            if k < len(vec):
                parts.append(vec[k] * CENTRE)
            out.append(total(parts))
        return out

    def dot(one, two):
        return total(x * y for x, y in zip(one, two))

    first = jnp.sqrt(gram[0][0] + GUARD)
    inv_first = 1.0 / first
    basis = [[inv_first]]
    images = [[gram[k][0] * inv_first for k in range(NUM)]]
    cosines, sines, upper = [], [], []
    target = [first]
    for col in range(ITERS):
        work = shifted(basis[col])
        image = [dot(work, gram[k]) for k in range(NUM)]
        coeffs = [dot(basis[i], image) for i in range(col + 1)]
        work = [
            total([work[k]] + [-(coeffs[i] * basis[i][k]) for i in range(col + 1) if k < len(basis[i])])
            for k in range(len(work))
        ]
        image = [total([image[k]] + [-(coeffs[i] * images[i][k]) for i in range(col + 1)]) for k in range(NUM)]
        subdiag = jnp.sqrt(jnp.maximum(dot(work, image), 0.0) + GUARD)
        if col + 1 < ITERS:
            scale = 1.0 / subdiag
            basis.append([x * scale for x in work])
            images.append([x * scale for x in image])
        column = list(coeffs)
        for k in range(col):
            a, b = column[k], column[k + 1]
            column[k] = cosines[k] * a + sines[k] * b
            column[k + 1] = cosines[k] * b - sines[k] * a
        a, b = column[col], subdiag
        radius = jnp.sqrt(a * a + b * b)
        inv_radius = 1.0 / radius
        cosines.append(a * inv_radius)
        sines.append(b * inv_radius)
        column[col] = radius
        upper.append((column, inv_radius))
        last = target[col]
        target[col] = cosines[col] * last
        target.append(-(sines[col] * last))
    weights = [None] * ITERS
    for col in reversed(range(ITERS)):
        rest = [target[col]] + [-(upper[k][0][col] * weights[k]) for k in range(col + 1, ITERS)]
        weights[col] = total(rest) * upper[col][1]
    coef = [total([weights[j] * basis[j][k] for j in range(k, ITERS)]) for k in range(ITERS)]
    return coef, shifted(coef)


def final_kernel(*refs):
    p_refs = refs[:NUM]
    rows_ref, x_ref, r_ref, xv_ref, rv_ref, work_ref, sem = refs[NUM:]
    summed = jnp.sum(rows_ref[...], axis=0, keepdims=True)
    gram = [[None] * NUM for _ in range(NUM)]
    for n, (i, j) in enumerate(PAIRS):
        gram[i][j] = gram[j][i] = jnp.broadcast_to(summed[:, n : n + 1], (8, 128))
    coef, image = small_solve(gram)
    for k in range(ITERS):
        work_ref[k] = coef[k]
    work_ref[ITERS] = 1.0 - image[0]
    for k in range(1, NUM):
        work_ref[ITERS + k] = -image[k]
    copies = []
    for b in range(ROWS // 8):
        rows = slice(8 * b, 8 * b + 8)
        for c in range(2):
            for t in range(2):
                xs = rs = None
                for k in range(NUM):
                    vec = p_refs[k][RIM + 8 * b : RIM + 8 * b + 8, 8 * c : 8 * c + 8, 128 * t : 128 * t + 128]
                    part = vec * work_ref[ITERS + k]
                    rs = part if rs is None else rs + part
                    if k < ITERS:
                        part = vec * work_ref[k]
                        xs = part if xs is None else xs + part
                where = (slice(8 * c, 8 * c + 8), rows, slice(128 * t, 128 * t + 128))
                xv_ref[where] = jnp.swapaxes(xs, 0, 1)
                rv_ref[where] = jnp.swapaxes(rs, 0, 1)
        for n, (src, dst) in enumerate(((xv_ref, x_ref), (rv_ref, r_ref))):
            copy = pltpu.make_async_copy(src.at[:, rows], dst.at[:, rows], sem.at[2 * b + n])
            copy.start()
            copies.append(copy)
    for copy in copies:
        copy.wait()


def diffusion_table(lat_total):
    row = np.arange(-RIM, lat_total + RIM, dtype=np.float64)
    phi = -math.pi / 2 + (row + 0.5) * (math.pi / lat_total)
    kx = DIFF_LON / (np.cos(phi) ** 2 + 0.1)
    kx = np.where((row >= 0) & (row < lat_total), kx, 0.0)
    return np.repeat(kx[:, None], 128, axis=1).astype(np.float32)


VMEM = pl.BlockSpec(memory_space=pltpu.VMEM)
HBM = pl.BlockSpec(memory_space=pltpu.HBM)


def shape(*dims):
    return jax.ShapeDtypeStruct(dims, F32)


def pairing(count, odd, closed):
    pairs = []
    for i in range(count):
        partner = i + 1 if (i % 2 == 0) != odd else i - 1
        if closed:
            partner %= count
        if 0 <= partner < count:
            pairs.append((i, partner))
    return pairs


def per_device(forcing, damping, coupling, wind_lon, wind_lat, *, nx, ny):
    inputs = (forcing, damping, wind_lon, wind_lat, coupling, jnp.asarray(diffusion_table(ny * ROWS)))
    s1, s2, x1, x2, couple, k_rows = pl.pallas_call(
        pack_kernel,
        in_specs=[HBM] * 6,
        out_specs=[VMEM] * 6,
        out_shape=[shape(34, 16, COLS)] * 2
        + [shape(2, 72, 128)] * 2
        + [shape(CH, CH), shape(EXT_ROWS, 128)],
        scratch_shapes=[
            pltpu.VMEM((CH, ROWS, COLS), F32),
            pltpu.VMEM((CH, ROWS, COLS), F32),
            pltpu.VMEM((ROWS, COLS), F32),
            pltpu.VMEM((ROWS, COLS), F32),
            pltpu.SemaphoreType.DMA((6,)),
        ],
        compiler_params=pltpu.CompilerParams(vmem_limit_bytes=8 * 2**20),
        name="pack",
    )(*(pltpu.with_memory_space_constraint(x, pltpu.HBM) for x in inputs))
    r1 = lax.ppermute(s1, "gy", pairing(ny, False, False))
    r2 = lax.ppermute(s2, "gy", pairing(ny, True, False))
    g1 = lax.ppermute(x1, "gx", pairing(nx, False, True))
    g2 = lax.ppermute(x2, "gx", pairing(nx, True, True))
    field = shape(EXT_ROWS, CH, EXT_COLS)
    mix = [pltpu.VMEM((8, CH, EXT_COLS), F32)] * 2
    carried = [field] * (INNER_STEPS + 2) + [shape(6, EXT_ROWS, EXT_COLS)]
    *state, k1, k2, kron = pl.pallas_call(
        inner_kernel,
        in_specs=[VMEM] * 6,
        out_specs=[VMEM] * (len(carried) + 3),
        out_shape=carried + [shape(2, 72, 128)] * 2 + [shape(8 * CH, 8 * CH)],
        scratch_shapes=mix,
        compiler_params=pltpu.CompilerParams(vmem_limit_bytes=8 * 2**20),
        cost_estimate=pl.CostEstimate(flops=10**8, bytes_accessed=2**20, transcendentals=0),
        name="inner",
    )(s1, s2, g1, g2, couple, k_rows)
    c1 = lax.ppermute(k1, "gy", pairing(ny, False, False))
    c2 = lax.ppermute(k2, "gy", pairing(ny, True, False))
    extra = [field] * (NUM - INNER_STEPS - 1)
    results = pl.pallas_call(
        outer_kernel,
        in_specs=[VMEM] * (6 + len(carried)),
        out_specs=[VMEM] * (len(carried) + len(extra) + 1),
        out_shape=carried + extra + [shape(128, 128)],
        input_output_aliases={6 + n: n for n in range(len(carried))},
        scratch_shapes=mix + [pltpu.VMEM((128, 128), F32)],
        compiler_params=pltpu.CompilerParams(vmem_limit_bytes=8 * 2**20),
        name="outer",
    )(r1, r2, c1, c2, k_rows, kron, *state)
    basis = results[: INNER_STEPS + 1] + results[len(carried) : -1]
    rows = lax.all_to_all(results[-1], ("gx", "gy"), 0, 0, tiled=True)
    return pl.pallas_call(
        final_kernel,
        in_specs=[VMEM] * (NUM + 1),
        out_specs=[HBM, HBM],
        out_shape=[shape(CH, ROWS, COLS)] * 2,
        scratch_shapes=[
            pltpu.VMEM((CH, ROWS, COLS), F32),
            pltpu.VMEM((CH, ROWS, COLS), F32),
            pltpu.VMEM((ITERS + NUM, 8, 128), F32),
            pltpu.SemaphoreType.DMA((ROWS // 4,)),
        ],
        compiler_params=pltpu.CompilerParams(vmem_limit_bytes=8 * 2**20),
        name="finish",
    )(*basis, rows)


def solution(mesh):
    spec = P(None, "gy", "gx")
    flat = P("gy", "gx")
    return jax.shard_map(
        functools.partial(per_device, nx=mesh.shape["gx"], ny=mesh.shape["gy"]),
        mesh=mesh,
        in_specs=(spec, spec, P(), flat, flat),
        out_specs=(spec, spec),
        check_vma=False,
    )
```

```python
import functools
import math

import jax
import jax.numpy as jnp
import numpy as np
from jax import lax
from jax.experimental import pallas as pl
from jax.experimental.pallas import tpu as pltpu
from jax.sharding import PartitionSpec as P


ITERS = 8
CH = 16
ROWS = 32
COLS = 256
RIM = 2 * ITERS
EXT_ROWS = ROWS + 2 * RIM
COUPLE = 0.25
DIFF_LAT = 0.5
DIFF_LON = 0.5
GUARD = 1.0

LOW, HIGH = 1.5, 26.0
CENTRE = (LOW + HIGH) / 2
SCALE = 4.0 / (HIGH - LOW)
NUM = ITERS + 1
PAIRS = [(i, j) for j in range(NUM) for i in range(j + 1)]
F32 = jnp.float32


def pack_kernel(
    f_hbm, d_hbm, wl_hbm, wt_hbm, cp_hbm, tab_hbm,
    s1_ref, s2_ref, x1_ref, x2_ref, cp_ref, k_ref,
    f_ref, d_ref, wl_ref, wt_ref, sem,
):
    start = pl.multiple_of(lax.axis_index("gy") * ROWS, ROWS)
    copies = [
        pltpu.make_async_copy(src, dst, sem.at[n])
        for n, (src, dst) in enumerate(
            (
                (f_hbm, f_ref), (d_hbm, d_ref), (wl_hbm, wl_ref), (wt_hbm, wt_ref),
                (cp_hbm, cp_ref), (tab_hbm.at[pl.ds(start, EXT_ROWS)], k_ref),
            )
        )
    ]
    for copy in copies:
        copy.start()
    for copy in copies:
        copy.wait()
    par_y = lax.rem(lax.axis_index("gy"), 2)
    par_x = lax.rem(lax.axis_index("gx"), 2)
    for ref, half in ((s1_ref, 1 - par_y), (s2_ref, par_y)):
        for q in range(2):
            off = pl.multiple_of(half * 16 + 8 * q, 8)
            for src, base in ((f_ref, 0), (d_ref, 16)):
                for c in range(2):
                    ref[base + 8 * q : base + 8 * q + 8, 8 * c : 8 * c + 8, :] = jnp.swapaxes(
                        src[8 * c : 8 * c + 8, pl.ds(off, 8), :], 0, 1
                    )
        off = pl.multiple_of(half * 16, 16)
        ref[32] = wl_ref[pl.ds(off, 16), :]
        ref[33] = wt_ref[pl.ds(off, 16), :]
    group = lax.broadcasted_iota(jnp.int32, (8, 128), 1) // 16

    def gather(tiles):
        left = jnp.zeros((8, 128), F32)
        right = jnp.zeros((8, 128), F32)
        for g, (low, high) in enumerate(tiles):
            left = jnp.where(group == g, pltpu.roll(low, 16 * g, 1) if g else low, left)
            shift = (16 * g + 16) % 128
            right = jnp.where(group == g, pltpu.roll(high, shift, 1) if shift else high, right)
        return jnp.where(par_x == 0, right, left), jnp.where(par_x == 0, left, right)

    winds = gather(
        [
            (ref[8 * q : 8 * q + 8, :128], ref[8 * q : 8 * q + 8, 128:])
            for ref in (wl_ref, wt_ref)
            for q in range(4)
        ]
    )
    for half in range(2):
        slot = 0
        for base in (0, 16):
            for q in range(2):
                for c in range(2):
                    tiles = []
                    for g in range(8):
                        row = base + 8 * q + g
                        pick = []
                        for t in range(2):
                            one = s1_ref[row, 8 * c : 8 * c + 8, 128 * t : 128 * t + 128]
                            two = s2_ref[row, 8 * c : 8 * c + 8, 128 * t : 128 * t + 128]
                            pick.append(jnp.where(par_y == half, two, one))
                        tiles.append(tuple(pick))
                    first, second = gather(tiles)
                    x1_ref[half, 8 * slot : 8 * slot + 8, :] = first
                    x2_ref[half, 8 * slot : 8 * slot + 8, :] = second
                    slot += 1
        x1_ref[half, 64:72, :] = winds[0]
        x2_ref[half, 64:72, :] = winds[1]


HALF = EXT_ROWS // 2
GHOST = 2
WIDE = 2 * COLS + 128
TILES = [slice(128 * t, 128 * t + 128) for t in range(5)]


def place_pairs(low, high, low_sides, high_sides, low_half, base, p0_ref, d_ref, coef_refs, k_ref):
    par_x = lax.rem(lax.axis_index("gx"), 2)
    lane = lax.broadcasted_iota(jnp.int32, (8, 128), 1)
    turned = jnp.logical_and(lane >= 48, lane < 80)
    coef_low, coef_high, coef_edge = coef_refs

    def turn(x, by):
        return pltpu.roll(x, by % 128, 1) if by % 128 else x

    def sides(reader, slot):
        a, b = reader(slot)
        return jnp.where(par_x == 0, a, b), jnp.where(par_x == 0, b, a)

    def spread(low_pair, low_group, high_pair, high_group):
        out = jnp.where(lane < 16, turn(low_pair[0], -16 * low_group), 0.0)
        out = jnp.where(lane >= 112, turn(low_pair[1], 112 - 16 * low_group), out)
        upper = jnp.where(lane >= 64, turn(high_pair[0], 64 - 16 * high_group), turn(high_pair[1], 48 - 16 * high_group))
        return jnp.where(turned, upper, out)

    scales = {}
    edges = {}
    wind_sides = (sides(low_sides, 8), sides(high_sides, 8))
    for side, (reader, half, sign, first) in enumerate(
        ((low, low_half, 1.0, base), (high, 1 - low_half, -1.0, EXT_ROWS - base - 16))
    ):
        for q in range(2):
            k = k_ref[first + 8 * q : first + 8 * q + 8]
            live = jnp.where(k > 0.0, 1.0, 0.0)
            kx = k * SCALE
            half_lat = live * (SCALE * DIFF_LAT)
            scales[side, q] = (live * SCALE, live * (SCALE * (1.0 + 2.0 * DIFF_LAT - CENTRE)) + 2.0 * kx)
            for t in range(3):
                winds = []
                for field in range(2):
                    if t < 2:
                        wind = reader(32 + field, slice(8 * q, 8 * q + 8), TILES[t])
                        if side:
                            wind = turn(wind, 64)
                    else:
                        group = 4 * field + 2 * half + q
                        east, west = wind_sides[side]
                        if side:
                            wind = jnp.where(lane >= 64, turn(east, 64 - 16 * group), turn(west, 48 - 16 * group))
                        else:
                            wind = jnp.where(lane < 64, turn(east, -16 * group), turn(west, 112 - 16 * group))
                    winds.append(wind * (live * (SCALE / 12.0)))
                lon, lat = winds[0], winds[1] * sign
                values = (
                    8.0 * lon - kx, -8.0 * lon - kx, -lon,
                    8.0 * lat - half_lat, -8.0 * lat - half_lat, -lat,
                )
                for n, value in enumerate(values):
                    if t == 2:
                        edges[side, q, n] = value
                    elif side:
                        row = first - HALF + 8 * q
                        coef_high[n, row : row + 8, TILES[t]] = value
                    else:
                        coef_low[n, first + 8 * q : first + 8 * q + 8, TILES[t]] = value
    inside = jnp.logical_or(lane < 16, lane >= 112)[:1]
    turned_row = turned[:1]
    for i in range(16):
        u = base + i
        j = 15 - i
        for n in range(6):
            a = edges[0, i // 8, n][i % 8 : i % 8 + 1]
            b = edges[1, j // 8, n][j % 8 : j % 8 + 1]
            coef_edge[n, u : u + 1, :] = jnp.where(turned_row, b, jnp.where(inside, a, 0.0))
    for c in range(2):
        subs = slice(8 * c, 8 * c + 8)
        pairs = {}
        for kind in range(2):
            for q in range(2):
                pairs[kind, 0, q] = sides(low_sides, 4 * kind + 2 * q + c)
                pairs[kind, 1, q] = sides(high_sides, 4 * kind + 2 * q + c)
        for i in range(16):
            u = base + i
            j = 15 - i
            mul_l, add_l = (x[i % 8 : i % 8 + 1] for x in scales[0, i // 8])
            mul_h, add_h = (x[j % 8 : j % 8 + 1] for x in scales[1, j // 8])
            for t in range(2):
                p0_ref[u, subs, TILES[t]] = low(i, subs, TILES[t])
                p0_ref[u, subs, TILES[2 + t]] = turn(high(j, subs, TILES[t]), 64)
                d_ref[u, subs, TILES[t]] = low(16 + i, subs, TILES[t]) * mul_l + add_l
                d_ref[u, subs, TILES[2 + t]] = turn(high(16 + j, subs, TILES[t]), 64) * mul_h + add_h
            f_edge, d_edge = (
                spread(pairs[kind, 0, i // 8], i % 8, pairs[kind, 1, j // 8], j % 8) for kind in range(2)
            )
            p0_ref[u, subs, TILES[4]] = f_edge
            mul = jnp.where(turned_row, mul_h, mul_l)
            add = jnp.where(turned_row, add_h, add_l)
            d_ref[u, subs, TILES[4]] = d_edge * mul + add


def mirror(p_ref):
    for g in range(GHOST):
        for dst, src in zip((0, 1, 2, 3, 4), (2, 3, 0, 1, 4)):
            p_ref[HALF + g, :, TILES[dst]] = pltpu.roll(p_ref[HALF - 1 - g, :, TILES[src]], 64, 1)


def split_kron(kron_ref):
    kron = kron_ref[...]
    hi = kron.astype(jnp.bfloat16)
    return hi, (kron - hi.astype(F32)).astype(jnp.bfloat16)


def run_blocks(blocks, p_refs, d_ref, coef_refs, kron, mix_refs):
    lane = lax.broadcasted_iota(jnp.int32, (CH, 128), 1)
    coef_low, coef_high, coef_edge = coef_refs

    def width(step):
        return WIDE if step < ITERS else 2 * COLS

    def mix(index):
        step, u0, count = blocks[index]
        size = count * CH
        kron_hi, kron_lo = (k[:size, :size] for k in kron)
        flat = p_refs[step - 1][u0 : u0 + count, :, : width(step)].reshape(size, width(step))
        hi = flat.astype(jnp.bfloat16)
        lo = (flat - hi.astype(F32)).astype(jnp.bfloat16)
        mixed = jnp.dot(kron_hi, hi, preferred_element_type=F32)
        mixed = mixed + jnp.dot(kron_hi, lo, preferred_element_type=F32)
        mixed = mixed + jnp.dot(kron_lo, hi, preferred_element_type=F32)
        mix_refs[index % 2][:count, :, : width(step)] = mixed.reshape(count, CH, width(step))

    def shifted(tiles, by):
        rolled = [pltpu.roll(x, by % 128, 1) for x in tiles]
        if by < 0:
            low, high = lane >= 128 + by, jnp.logical_and(lane >= 64 + by, lane < 64)
            nexts = (1, 4, 3, 4)
        else:
            low, high = lane < by, jnp.logical_and(lane >= 64, lane < 64 + by)
            nexts = (4, 0, 4, 2)
        ends = (0, 2) if by < 0 else (1, 3)
        out = [jnp.where(low if t < 2 else high, rolled[nexts[t]], rolled[t]) for t in range(4)]
        out.append(jnp.where(low, rolled[ends[0]], jnp.where(high, rolled[ends[1]], rolled[4])))
        return out

    mix(0)
    for index, (step, u0, count) in enumerate(blocks):
        more = index + 1 < len(blocks)
        late = False
        if more:
            step_n, u_n, count_n = blocks[index + 1]
            late = step_n == step + 1 and u_n < u0 + count and u0 < u_n + count_n
        if more and not late:
            mix(index + 1)
        src, dst = p_refs[step - 1], p_refs[step]
        for i in range(count):
            u = u0 + i
            centre = [src[u, :, t] for t in TILES]
            east, west = shifted(centre, -1), shifted(centre, 1)
            east2, west2 = shifted(centre, -2), shifted(centre, 2)
            for t in range(width(step) // 128):
                at = TILES[t]
                if t < 2:
                    coef = [coef_low[n, u : u + 1, at] for n in range(6)]
                elif t < 4:
                    v = HALF - 1 - u
                    coef = [coef_high[n, v : v + 1, TILES[t - 2]] for n in range(6)]
                else:
                    coef = [coef_edge[n, u : u + 1, :] for n in range(6)]
                acc = mix_refs[index % 2][i, :, at] + d_ref[u, :, at] * centre[t]
                if step > 1:
                    acc = acc - p_refs[step - 2][u, :, at]
                acc = acc + coef[0] * east[t]
                acc = acc + coef[1] * west[t]
                acc = acc + coef[2] * (east2[t] - west2[t])
                acc = acc + coef[3] * src[u + 1, :, at]
                acc = acc + coef[4] * src[u - 1, :, at]
                acc = acc + coef[5] * (src[u + 2, :, at] - src[u - 2, :, at])
                dst[u, :, at] = acc
        if u0 + count == HALF and step < ITERS:
            mirror(dst)
        if late:
            mix(index + 1)


INNER_STEPS = 6
INNER = []
OUTER = []
for _j in range(1, NUM):
    _edge = RIM + 2 * _j
    if _j <= INNER_STEPS:
        _rest = HALF - _edge
        if _rest > 8:
            INNER.append((_j, _edge + 8, _rest - 8))
        INNER.append((_j, _edge, min(_rest, 8)))
        OUTER += [(_j, 2 * _j + 8, 8), (_j, 2 * _j, 8)]
    elif _j < ITERS:
        OUTER += [(_j, 26, 6), (_j, 20, 6), (_j, 14, 6)]
    else:
        OUTER += [(_j, 24, 8), (_j, 16, 8)]


def corner_kernel(g1_ref, g2_ref, k1_ref, k2_ref):
    par_y = lax.rem(lax.axis_index("gy"), 2)
    for n, g_ref in enumerate((g1_ref, g2_ref)):
        k1_ref[n] = g_ref[1 - par_y]
        k2_ref[n] = g_ref[par_y]


def inner_kernel(s1_ref, s2_ref, g1_ref, g2_ref, cp_ref, k_ref, *refs):
    p_refs = refs[: INNER_STEPS + 1]
    d_ref, *coef_refs = refs[INNER_STEPS + 1 : INNER_STEPS + 5]
    kron_ref, *mix_refs = refs[INNER_STEPS + 5 :]
    par_y = lax.rem(lax.axis_index("gy"), 2)
    size = 8 * CH
    pick = lax.broadcasted_iota(jnp.int32, (size, CH), 0) % CH
    pick = (pick == lax.broadcasted_iota(jnp.int32, (size, CH), 1)).astype(F32)
    tall = jnp.dot(
        pick, cp_ref[...] * (COUPLE * SCALE), precision=lax.Precision.HIGHEST, preferred_element_type=F32
    )
    full = lax.dot_general(
        tall, pick, (((1,), (1,)), ((), ())), precision=lax.Precision.HIGHEST, preferred_element_type=F32
    )
    row = lax.broadcasted_iota(jnp.int32, (size, size), 0) // CH
    col = lax.broadcasted_iota(jnp.int32, (size, size), 1) // CH
    kron_ref[...] = jnp.where(row == col, full, 0.0)
    place_pairs(
        lambda *at: jnp.where(par_y == 0, s2_ref[at], s1_ref[at]),
        lambda *at: jnp.where(par_y == 0, s1_ref[at], s2_ref[at]),
        lambda slot: (g1_ref[0, 8 * slot : 8 * slot + 8], g2_ref[0, 8 * slot : 8 * slot + 8]),
        lambda slot: (g1_ref[1, 8 * slot : 8 * slot + 8], g2_ref[1, 8 * slot : 8 * slot + 8]),
        0, RIM, p_refs[0], d_ref, coef_refs, k_ref,
    )
    mirror(p_refs[0])
    run_blocks(INNER, p_refs, d_ref, coef_refs, split_kron(kron_ref), mix_refs)


def outer_kernel(r1_ref, r2_ref, c1_ref, c2_ref, k_ref, kron_ref, *refs):
    count = INNER_STEPS + 5
    refs = refs[count:]
    p_refs = refs[: INNER_STEPS + 1] + refs[count : count + NUM - INNER_STEPS - 1]
    d_ref, coef_refs = refs[INNER_STEPS + 1], refs[INNER_STEPS + 2 : count]
    gram_ref, mix_a, mix_b, sums_ref = refs[count + NUM - INNER_STEPS - 1 :]
    par_y = lax.rem(lax.axis_index("gy"), 2)

    def corners(one, two):
        def read(slot):
            at = slice(8 * slot, 8 * slot + 8)
            return tuple(jnp.where(par_y == 0, one[n, at], two[n, at]) for n in range(2))

        return read

    place_pairs(
        lambda *at: jnp.where(par_y == 0, r2_ref[at], r1_ref[at]),
        lambda *at: jnp.where(par_y == 0, r1_ref[at], r2_ref[at]),
        corners(c2_ref, c1_ref), corners(c1_ref, c2_ref),
        1, 0, p_refs[0], d_ref, coef_refs, k_ref,
    )
    run_blocks(OUTER, p_refs, d_ref, coef_refs, split_kron(kron_ref), (mix_a, mix_b))

    sums_ref[...] = jnp.zeros_like(sums_ref)
    for lo_k, hi_k in ((0, 6), (6, NUM)):
        pairs = [(n, i, j) for n, (i, j) in enumerate(PAIRS) if lo_k <= j < hi_k]

        def body(r, accs, pairs=pairs, hi_k=hi_k):
            accs = list(accs)
            for c in range(2):
                for t in range(4):
                    vecs = [p_refs[k][RIM + r, 8 * c : 8 * c + 8, TILES[t]] for k in range(hi_k)]
                    for n, (_, i, j) in enumerate(pairs):
                        accs[n] = accs[n] + vecs[i] * vecs[j]
            return tuple(accs)

        accs = lax.fori_loop(0, ROWS // 2, body, tuple(jnp.zeros((8, 128), F32) for _ in pairs))
        for (n, _, _), acc in zip(pairs, accs):
            sums_ref[n : n + 1, :] = jnp.sum(acc, axis=0, keepdims=True)
    gram_ref[...] = lax.dot_general(
        jnp.ones((128, 128), F32), sums_ref[...], (((1,), (1,)), ((), ())),
        precision=lax.Precision.HIGHEST, preferred_element_type=F32,
    )


def small_solve(gram):
    inv = 1.0 / SCALE

    def total(values):
        values = list(values)
        while len(values) > 1:
            nxt = [values[k] + values[k + 1] for k in range(0, len(values) - 1, 2)]
            if len(values) % 2:
                nxt.append(values[-1])
            values = nxt
        return values[0]

    def shifted(vec):
        out = []
        for k in range(len(vec) + 1):
            terms = [vec[m] for m in (k - 1, k + 1) if 0 <= m < len(vec)]
            parts = [total(terms) * inv] if terms else []
            if k < len(vec):
                parts.append(vec[k] * CENTRE)
            out.append(total(parts))
        return out

    def dot(one, two):
        return total(x * y for x, y in zip(one, two))

    first = jnp.sqrt(gram[0][0] + GUARD)
    inv_first = 1.0 / first
    basis = [[inv_first]]
    images = [[gram[k][0] * inv_first for k in range(NUM)]]
    cosines, sines, upper = [], [], []
    target = [first]
    for col in range(ITERS):
        work = shifted(basis[col])
        image = [dot(work, gram[k]) for k in range(NUM)]
        coeffs = [dot(basis[i], image) for i in range(col + 1)]
        work = [
            total([work[k]] + [-(coeffs[i] * basis[i][k]) for i in range(col + 1) if k < len(basis[i])])
            for k in range(len(work))
        ]
        image = [total([image[k]] + [-(coeffs[i] * images[i][k]) for i in range(col + 1)]) for k in range(NUM)]
        subdiag = jnp.sqrt(jnp.maximum(dot(work, image), 0.0) + GUARD)
        if col + 1 < ITERS:
            scale = 1.0 / subdiag
            basis.append([x * scale for x in work])
            images.append([x * scale for x in image])
        column = list(coeffs)
        for k in range(col):
            a, b = column[k], column[k + 1]
            column[k] = cosines[k] * a + sines[k] * b
            column[k + 1] = cosines[k] * b - sines[k] * a
        a, b = column[col], subdiag
        radius = jnp.sqrt(a * a + b * b)
        inv_radius = 1.0 / radius
        cosines.append(a * inv_radius)
        sines.append(b * inv_radius)
        column[col] = radius
        upper.append((column, inv_radius))
        last = target[col]
        target[col] = cosines[col] * last
        target.append(-(sines[col] * last))
    weights = [None] * ITERS
    for col in reversed(range(ITERS)):
        rest = [target[col]] + [-(upper[k][0][col] * weights[k]) for k in range(col + 1, ITERS)]
        weights[col] = total(rest) * upper[col][1]
    coef = [total([weights[j] * basis[j][k] for j in range(k, ITERS)]) for k in range(ITERS)]
    return coef, shifted(coef)


def final_kernel(*refs):
    p_refs = refs[:NUM]
    rows_ref, x_ref, r_ref, xv_ref, rv_ref, work_ref, sem = refs[NUM:]
    summed = jnp.sum(rows_ref[...], axis=0, keepdims=True)
    gram = [[None] * NUM for _ in range(NUM)]
    for n, (i, j) in enumerate(PAIRS):
        gram[i][j] = gram[j][i] = jnp.broadcast_to(summed[:, n : n + 1], (8, 128))
    coef, image = small_solve(gram)
    for k in range(ITERS):
        work_ref[k] = coef[k]
    work_ref[ITERS] = 1.0 - image[0]
    for k in range(1, NUM):
        work_ref[ITERS + k] = -image[k]
    copies = []
    for b in range(ROWS // 8):
        rows = slice(8 * b, 8 * b + 8)
        for c in range(2):
            for t in range(2):
                upper = b >= 2
                first = HALF - 1 - 8 * (b - 2) - 7 if upper else RIM + 8 * b
                tile = TILES[2 + t] if upper else TILES[t]
                xs = rs = None
                for k in range(NUM):
                    vec = p_refs[k][first : first + 8, 8 * c : 8 * c + 8, tile]
                    part = vec * work_ref[ITERS + k]
                    rs = part if rs is None else rs + part
                    if k < ITERS:
                        part = vec * work_ref[k]
                        xs = part if xs is None else xs + part
                where = (slice(8 * c, 8 * c + 8), rows, slice(128 * t, 128 * t + 128))
                for ref, value in ((xv_ref, xs), (rv_ref, rs)):
                    if upper:
                        value = jnp.stack([pltpu.roll(value[7 - i], 64, 1) for i in range(8)])
                    ref[where] = jnp.swapaxes(value, 0, 1)
        for n, (src, dst) in enumerate(((xv_ref, x_ref), (rv_ref, r_ref))):
            copy = pltpu.make_async_copy(src.at[:, rows], dst.at[:, rows], sem.at[2 * b + n])
            copy.start()
            copies.append(copy)
    for copy in copies:
        copy.wait()


def diffusion_table(lat_total):
    row = np.arange(-RIM, lat_total + RIM, dtype=np.float64)
    phi = -math.pi / 2 + (row + 0.5) * (math.pi / lat_total)
    kx = DIFF_LON / (np.cos(phi) ** 2 + 0.1)
    kx = np.where((row >= 0) & (row < lat_total), kx, 0.0)
    return np.repeat(kx[:, None], 128, axis=1).astype(np.float32)


VMEM = pl.BlockSpec(memory_space=pltpu.VMEM)
HBM = pl.BlockSpec(memory_space=pltpu.HBM)


def shape(*dims):
    return jax.ShapeDtypeStruct(dims, F32)


def pairing(count, odd, closed):
    pairs = []
    for i in range(count):
        partner = i + 1 if (i % 2 == 0) != odd else i - 1
        if closed:
            partner %= count
        if 0 <= partner < count:
            pairs.append((i, partner))
    return pairs


def per_device(forcing, damping, coupling, wind_lon, wind_lat, *, nx, ny):
    inputs = (forcing, damping, wind_lon, wind_lat, coupling, jnp.asarray(diffusion_table(ny * ROWS)))
    s1, s2, x1, x2, couple, k_rows = pl.pallas_call(
        pack_kernel,
        in_specs=[HBM] * 6,
        out_specs=[VMEM] * 6,
        out_shape=[shape(34, 16, COLS)] * 2
        + [shape(2, 72, 128)] * 2
        + [shape(CH, CH), shape(EXT_ROWS, 128)],
        scratch_shapes=[
            pltpu.VMEM((CH, ROWS, COLS), F32),
            pltpu.VMEM((CH, ROWS, COLS), F32),
            pltpu.VMEM((ROWS, COLS), F32),
            pltpu.VMEM((ROWS, COLS), F32),
            pltpu.SemaphoreType.DMA((6,)),
        ],
        compiler_params=pltpu.CompilerParams(vmem_limit_bytes=8 * 2**20),
        name="pack",
    )(*(pltpu.with_memory_space_constraint(x, pltpu.HBM) for x in inputs))
    r1 = lax.ppermute(s1, "gy", pairing(ny, False, False))
    r2 = lax.ppermute(s2, "gy", pairing(ny, True, False))
    g1 = lax.ppermute(x1, "gx", pairing(nx, False, True))
    g2 = lax.ppermute(x2, "gx", pairing(nx, True, True))
    k1, k2 = pl.pallas_call(
        corner_kernel,
        in_specs=[VMEM] * 2,
        out_specs=[VMEM] * 2,
        out_shape=[shape(2, 72, 128)] * 2,
        compiler_params=pltpu.CompilerParams(vmem_limit_bytes=2**20),
        name="corner",
    )(g1, g2)
    c1 = lax.ppermute(k1, "gy", pairing(ny, False, False))
    c2 = lax.ppermute(k2, "gy", pairing(ny, True, False))
    field = shape(HALF + GHOST, CH, WIDE)
    mix = [pltpu.VMEM((8, CH, WIDE), F32)] * 2
    carried = [field] * (INNER_STEPS + 1) + [shape(HALF, CH, WIDE)]
    carried += [shape(6, HALF, COLS)] * 2 + [shape(6, HALF, 128)]
    *state, kron = pl.pallas_call(
        inner_kernel,
        in_specs=[VMEM] * 6,
        out_specs=[VMEM] * (len(carried) + 1),
        out_shape=carried + [shape(8 * CH, 8 * CH)],
        scratch_shapes=mix,
        compiler_params=pltpu.CompilerParams(vmem_limit_bytes=8 * 2**20),
        cost_estimate=pl.CostEstimate(flops=10**8, bytes_accessed=2**20, transcendentals=0),
        name="inner",
    )(s1, s2, g1, g2, couple, k_rows)
    extra = [field] * (NUM - INNER_STEPS - 1)
    results = pl.pallas_call(
        outer_kernel,
        in_specs=[VMEM] * (6 + len(carried)),
        out_specs=[VMEM] * (len(carried) + len(extra) + 1),
        out_shape=carried + extra + [shape(128, 128)],
        input_output_aliases={6 + n: n for n in range(len(carried))},
        scratch_shapes=mix + [pltpu.VMEM((128, 128), F32)],
        compiler_params=pltpu.CompilerParams(vmem_limit_bytes=8 * 2**20),
        name="outer",
    )(r1, r2, c1, c2, k_rows, kron, *state)
    basis = results[: INNER_STEPS + 1] + results[len(carried) : -1]
    rows = lax.all_to_all(results[-1], ("gx", "gy"), 0, 0, tiled=True)
    return pl.pallas_call(
        final_kernel,
        in_specs=[VMEM] * (NUM + 1),
        out_specs=[HBM, HBM],
        out_shape=[shape(CH, ROWS, COLS)] * 2,
        scratch_shapes=[
            pltpu.VMEM((CH, ROWS, COLS), F32),
            pltpu.VMEM((CH, ROWS, COLS), F32),
            pltpu.VMEM((ITERS + NUM, 8, 128), F32),
            pltpu.SemaphoreType.DMA((ROWS // 4,)),
        ],
        compiler_params=pltpu.CompilerParams(vmem_limit_bytes=8 * 2**20),
        name="finish",
    )(*basis, rows)


def solution(mesh):
    spec = P(None, "gy", "gx")
    flat = P("gy", "gx")
    return jax.shard_map(
        functools.partial(per_device, nx=mesh.shape["gx"], ny=mesh.shape["gy"]),
        mesh=mesh,
        in_specs=(spec, spec, P(), flat, flat),
        out_specs=(spec, spec),
        check_vma=False,
    )
```

```python
import functools
import math

import jax
import jax.numpy as jnp
import numpy as np
from jax import lax
from jax.experimental import pallas as pl
from jax.experimental.pallas import tpu as pltpu
from jax.sharding import PartitionSpec as P


ITERS = 8
CH = 16
ROWS = 32
COLS = 256
RIM = 2 * ITERS
EXT_ROWS = ROWS + 2 * RIM
COUPLE = 0.25
DIFF_LAT = 0.5
DIFF_LON = 0.5
GUARD = 1.0

LOW, HIGH = 1.5, 26.0
CENTRE = (LOW + HIGH) / 2
SCALE = 4.0 / (HIGH - LOW)
NUM = ITERS + 1
PAIRS = [(i, j) for j in range(NUM) for i in range(j + 1)]
F32 = jnp.float32


def pack_kernel(
    f_hbm, d_hbm, wl_hbm, wt_hbm, cp_hbm, tab_hbm,
    s1_ref, s2_ref, x1_ref, x2_ref, cp_ref, k_ref,
    f_ref, d_ref, wl_ref, wt_ref, sem,
):
    start = pl.multiple_of(lax.axis_index("gy") * ROWS, ROWS)
    copies = [
        pltpu.make_async_copy(src, dst, sem.at[n])
        for n, (src, dst) in enumerate(
            (
                (f_hbm, f_ref), (d_hbm, d_ref), (wl_hbm, wl_ref), (wt_hbm, wt_ref),
                (cp_hbm, cp_ref), (tab_hbm.at[pl.ds(start, EXT_ROWS)], k_ref),
            )
        )
    ]
    for copy in copies:
        copy.start()
    for copy in copies:
        copy.wait()
    par_y = lax.rem(lax.axis_index("gy"), 2)
    par_x = lax.rem(lax.axis_index("gx"), 2)
    for ref, half in ((s1_ref, 1 - par_y), (s2_ref, par_y)):
        for q in range(2):
            off = pl.multiple_of(half * 16 + 8 * q, 8)
            for src, base in ((f_ref, 0), (d_ref, 16)):
                for c in range(2):
                    ref[base + 8 * q : base + 8 * q + 8, 8 * c : 8 * c + 8, :] = jnp.swapaxes(
                        src[8 * c : 8 * c + 8, pl.ds(off, 8), :], 0, 1
                    )
        off = pl.multiple_of(half * 16, 16)
        ref[32] = wl_ref[pl.ds(off, 16), :]
        ref[33] = wt_ref[pl.ds(off, 16), :]
    group = lax.broadcasted_iota(jnp.int32, (8, 128), 1) // 16

    def gather(tiles):
        left = jnp.zeros((8, 128), F32)
        right = jnp.zeros((8, 128), F32)
        for g, (low, high) in enumerate(tiles):
            left = jnp.where(group == g, pltpu.roll(low, 16 * g, 1) if g else low, left)
            shift = (16 * g + 16) % 128
            right = jnp.where(group == g, pltpu.roll(high, shift, 1) if shift else high, right)
        return jnp.where(par_x == 0, right, left), jnp.where(par_x == 0, left, right)

    winds = gather(
        [
            (ref[8 * q : 8 * q + 8, :128], ref[8 * q : 8 * q + 8, 128:])
            for ref in (wl_ref, wt_ref)
            for q in range(4)
        ]
    )
    for half in range(2):
        slot = 0
        for base in (0, 16):
            for q in range(2):
                for c in range(2):
                    tiles = []
                    for g in range(8):
                        row = base + 8 * q + g
                        pick = []
                        for t in range(2):
                            one = s1_ref[row, 8 * c : 8 * c + 8, 128 * t : 128 * t + 128]
                            two = s2_ref[row, 8 * c : 8 * c + 8, 128 * t : 128 * t + 128]
                            pick.append(jnp.where(par_y == half, two, one))
                        tiles.append(tuple(pick))
                    first, second = gather(tiles)
                    x1_ref[half, 8 * slot : 8 * slot + 8, :] = first
                    x2_ref[half, 8 * slot : 8 * slot + 8, :] = second
                    slot += 1
        x1_ref[half, 64:72, :] = winds[0]
        x2_ref[half, 64:72, :] = winds[1]


HALF = EXT_ROWS // 2
GHOST = 2
WIDE = 2 * COLS + 128
TILES = [slice(128 * t, 128 * t + 128) for t in range(5)]


def place_pairs(
    low, high, low_sides, high_sides, low_half, base, p0_ref, d_ref, coef_refs, k_ref, main=True, edge=True
):
    par_x = lax.rem(lax.axis_index("gx"), 2)
    lane = lax.broadcasted_iota(jnp.int32, (8, 128), 1)
    turned = jnp.logical_and(lane >= 48, lane < 80)
    coef_low, coef_high, coef_edge = coef_refs
    spans = [t for t in range(3) if (edge if t == 2 else main)]

    def turn(x, by):
        return pltpu.roll(x, by % 128, 1) if by % 128 else x

    def sides(reader, slot):
        a, b = reader(slot)
        return jnp.where(par_x == 0, a, b), jnp.where(par_x == 0, b, a)

    def spread(low_pair, low_group, high_pair, high_group):
        out = jnp.where(lane < 16, turn(low_pair[0], -16 * low_group), 0.0)
        out = jnp.where(lane >= 112, turn(low_pair[1], 112 - 16 * low_group), out)
        upper = jnp.where(lane >= 64, turn(high_pair[0], 64 - 16 * high_group), turn(high_pair[1], 48 - 16 * high_group))
        return jnp.where(turned, upper, out)

    scales = {}
    edges = {}
    wind_sides = (sides(low_sides, 8), sides(high_sides, 8)) if edge else None
    for side, (reader, half, sign, first) in enumerate(
        ((low, low_half, 1.0, base), (high, 1 - low_half, -1.0, EXT_ROWS - base - 16))
    ):
        for q in range(2):
            k = k_ref[first + 8 * q : first + 8 * q + 8]
            live = jnp.where(k > 0.0, 1.0, 0.0)
            kx = k * SCALE
            half_lat = live * (SCALE * DIFF_LAT)
            scales[side, q] = (live * SCALE, live * (SCALE * (1.0 + 2.0 * DIFF_LAT - CENTRE)) + 2.0 * kx)
            for t in spans:
                winds = []
                for field in range(2):
                    if t < 2:
                        wind = reader(32 + field, slice(8 * q, 8 * q + 8), TILES[t])
                        if side:
                            wind = turn(wind, 64)
                    else:
                        group = 4 * field + 2 * half + q
                        east, west = wind_sides[side]
                        if side:
                            wind = jnp.where(lane >= 64, turn(east, 64 - 16 * group), turn(west, 48 - 16 * group))
                        else:
                            wind = jnp.where(lane < 64, turn(east, -16 * group), turn(west, 112 - 16 * group))
                    winds.append(wind * (live * (SCALE / 12.0)))
                lon, lat = winds[0], winds[1] * sign
                values = (
                    8.0 * lon - kx, -8.0 * lon - kx, -lon,
                    8.0 * lat - half_lat, -8.0 * lat - half_lat, -lat,
                )
                for n, value in enumerate(values):
                    if t == 2:
                        edges[side, q, n] = value
                    elif side:
                        row = first - HALF + 8 * q
                        coef_high[n, row : row + 8, TILES[t]] = value
                    else:
                        coef_low[n, first + 8 * q : first + 8 * q + 8, TILES[t]] = value
    inside = jnp.logical_or(lane < 16, lane >= 112)[:1]
    turned_row = turned[:1]
    for i in range(16):
        u = base + i
        j = 15 - i
        for n in range(6 if edge else 0):
            a = edges[0, i // 8, n][i % 8 : i % 8 + 1]
            b = edges[1, j // 8, n][j % 8 : j % 8 + 1]
            coef_edge[n, u : u + 1, :] = jnp.where(turned_row, b, jnp.where(inside, a, 0.0))
    for c in range(2):
        subs = slice(8 * c, 8 * c + 8)
        pairs = {}
        for kind in range(2 if edge else 0):
            for q in range(2):
                pairs[kind, 0, q] = sides(low_sides, 4 * kind + 2 * q + c)
                pairs[kind, 1, q] = sides(high_sides, 4 * kind + 2 * q + c)
        for i in range(16):
            u = base + i
            j = 15 - i
            mul_l, add_l = (x[i % 8 : i % 8 + 1] for x in scales[0, i // 8])
            mul_h, add_h = (x[j % 8 : j % 8 + 1] for x in scales[1, j // 8])
            for t in range(2 if main else 0):
                p0_ref[u, subs, TILES[t]] = low(i, subs, TILES[t])
                p0_ref[u, subs, TILES[2 + t]] = turn(high(j, subs, TILES[t]), 64)
                d_ref[u, subs, TILES[t]] = low(16 + i, subs, TILES[t]) * mul_l + add_l
                d_ref[u, subs, TILES[2 + t]] = turn(high(16 + j, subs, TILES[t]), 64) * mul_h + add_h
            if not edge:
                continue
            f_edge, d_edge = (
                spread(pairs[kind, 0, i // 8], i % 8, pairs[kind, 1, j // 8], j % 8) for kind in range(2)
            )
            p0_ref[u, subs, TILES[4]] = f_edge
            mul = jnp.where(turned_row, mul_h, mul_l)
            add = jnp.where(turned_row, add_h, add_l)
            d_ref[u, subs, TILES[4]] = d_edge * mul + add


def mirror(p_ref):
    for g in range(GHOST):
        for dst, src in zip((0, 1, 2, 3, 4), (2, 3, 0, 1, 4)):
            p_ref[HALF + g, :, TILES[dst]] = pltpu.roll(p_ref[HALF - 1 - g, :, TILES[src]], 64, 1)


def split_kron(kron_ref):
    kron = kron_ref[...]
    hi = kron.astype(jnp.bfloat16)
    return hi, (kron - hi.astype(F32)).astype(jnp.bfloat16)


def run_blocks(blocks, p_refs, d_ref, coef_refs, kron, mix_refs):
    lane = lax.broadcasted_iota(jnp.int32, (8, 128), 1)
    coef_low, coef_high, coef_edge = coef_refs

    def width(step):
        return WIDE if step < ITERS else 2 * COLS

    def mix(index):
        step, u0, count = blocks[index]
        size = count * CH
        kron_hi, kron_lo = (k[:size, :size] for k in kron)
        flat = p_refs[step - 1][u0 : u0 + count, :, : width(step)].reshape(size, width(step))
        hi = flat.astype(jnp.bfloat16)
        lo = (flat - hi.astype(F32)).astype(jnp.bfloat16)
        mixed = jnp.dot(kron_hi, hi, preferred_element_type=F32)
        mixed = mixed + jnp.dot(kron_hi, lo, preferred_element_type=F32)
        mixed = mixed + jnp.dot(kron_lo, hi, preferred_element_type=F32)
        mix_refs[index % 2][:count, :, : width(step)] = mixed.reshape(count, CH, width(step))

    def shifted(tiles, by):
        rolled = [pltpu.roll(x, by % 128, 1) for x in tiles]
        if by < 0:
            low, high = lane >= 128 + by, jnp.logical_and(lane >= 64 + by, lane < 64)
            nexts = (1, 4, 3, 4)
        else:
            low, high = lane < by, jnp.logical_and(lane >= 64, lane < 64 + by)
            nexts = (4, 0, 4, 2)
        ends = (0, 2) if by < 0 else (1, 3)
        out = [jnp.where(low if t < 2 else high, rolled[nexts[t]], rolled[t]) for t in range(4)]
        out.append(jnp.where(low, rolled[ends[0]], jnp.where(high, rolled[ends[1]], rolled[4])))
        return out

    mix(0)
    for index, (step, u0, count) in enumerate(blocks):
        more = index + 1 < len(blocks)
        late = False
        if more:
            step_n, u_n, count_n = blocks[index + 1]
            late = step_n == step + 1 and u_n < u0 + count and u0 < u_n + count_n
        if more and not late:
            mix(index + 1)
        src, dst = p_refs[step - 1], p_refs[step]
        for i, s in [(i, s) for i in range(count) for s in (slice(0, 8), slice(8, 16))]:
            u = u0 + i
            centre = [src[u, s, t] for t in TILES]
            east, west = shifted(centre, -1), shifted(centre, 1)
            east2, west2 = shifted(centre, -2), shifted(centre, 2)
            span = range(width(step) // 128)

            def coef(n):
                out = []
                for t in span:
                    if t < 2:
                        out.append(coef_low[n, u : u + 1, TILES[t]])
                    elif t < 4:
                        v = HALF - 1 - u
                        out.append(coef_high[n, v : v + 1, TILES[t - 2]])
                    else:
                        out.append(coef_edge[n, u : u + 1, :])
                return out

            acc = [mix_refs[index % 2][i, s, TILES[t]] + d_ref[u, s, TILES[t]] * centre[t] for t in span]
            if step > 1:
                acc = [acc[t] - p_refs[step - 2][u, s, TILES[t]] for t in span]
            for n, values in (
                (0, lambda t: east[t]),
                (1, lambda t: west[t]),
                (2, lambda t: east2[t] - west2[t]),
                (3, lambda t: src[u + 1, s, TILES[t]]),
                (4, lambda t: src[u - 1, s, TILES[t]]),
                (5, lambda t: src[u + 2, s, TILES[t]] - src[u - 2, s, TILES[t]]),
            ):
                scale = coef(n)
                acc = [acc[t] + scale[t] * values(t) for t in span]
            for t in span:
                dst[u, s, TILES[t]] = acc[t]
        if u0 + count == HALF and step < ITERS:
            mirror(dst)
        if late:
            mix(index + 1)


INNER_STEPS = 6
INNER = []
OUTER = []
for _j in range(1, NUM):
    _edge = RIM + 2 * _j
    if _j <= INNER_STEPS:
        _rest = HALF - _edge
        if _rest > 8:
            INNER.append((_j, _edge + 8, _rest - 8))
        INNER.append((_j, _edge, min(_rest, 8)))
        OUTER += [(_j, 2 * _j + 8, 8), (_j, 2 * _j, 8)]
    elif _j < ITERS:
        OUTER += [(_j, 26, 6), (_j, 20, 6), (_j, 14, 6)]
    else:
        OUTER += [(_j, 24, 8), (_j, 16, 8)]


def corner_kernel(g1_ref, g2_ref, k1_ref, k2_ref):
    par_y = lax.rem(lax.axis_index("gy"), 2)
    for n, g_ref in enumerate((g1_ref, g2_ref)):
        k1_ref[n] = g_ref[1 - par_y]
        k2_ref[n] = g_ref[par_y]


def stage_kernel(s1_ref, s2_ref, cp_ref, k_ref, p0_ref, d_ref, coef_low, coef_high, kron_ref):
    par_y = lax.rem(lax.axis_index("gy"), 2)
    size = 8 * CH
    pick = lax.broadcasted_iota(jnp.int32, (size, CH), 0) % CH
    pick = (pick == lax.broadcasted_iota(jnp.int32, (size, CH), 1)).astype(F32)
    tall = jnp.dot(
        pick, cp_ref[...] * (COUPLE * SCALE), precision=lax.Precision.HIGHEST, preferred_element_type=F32
    )
    full = lax.dot_general(
        tall, pick, (((1,), (1,)), ((), ())), precision=lax.Precision.HIGHEST, preferred_element_type=F32
    )
    row = lax.broadcasted_iota(jnp.int32, (size, size), 0) // CH
    col = lax.broadcasted_iota(jnp.int32, (size, size), 1) // CH
    kron_ref[...] = jnp.where(row == col, full, 0.0)
    place_pairs(
        lambda *at: jnp.where(par_y == 0, s2_ref[at], s1_ref[at]),
        lambda *at: jnp.where(par_y == 0, s1_ref[at], s2_ref[at]),
        None, None, 0, RIM, p0_ref, d_ref, (coef_low, coef_high, None), k_ref, edge=False,
    )


def inner_kernel(g1_ref, g2_ref, k_ref, kron_ref, *refs):
    refs = refs[4:]
    p_refs = refs[: INNER_STEPS + 1]
    d_ref, *coef_refs = refs[INNER_STEPS + 1 : INNER_STEPS + 5]
    mix_refs = refs[INNER_STEPS + 5 :]
    place_pairs(
        None, None,
        lambda slot: (g1_ref[0, 8 * slot : 8 * slot + 8], g2_ref[0, 8 * slot : 8 * slot + 8]),
        lambda slot: (g1_ref[1, 8 * slot : 8 * slot + 8], g2_ref[1, 8 * slot : 8 * slot + 8]),
        0, RIM, p_refs[0], d_ref, coef_refs, k_ref, main=False,
    )
    mirror(p_refs[0])
    run_blocks(INNER, p_refs, d_ref, coef_refs, split_kron(kron_ref), mix_refs)


def outer_kernel(r1_ref, r2_ref, c1_ref, c2_ref, k_ref, kron_ref, *refs):
    count = INNER_STEPS + 5
    refs = refs[count:]
    p_refs = refs[: INNER_STEPS + 1] + refs[count : count + NUM - INNER_STEPS - 1]
    d_ref, coef_refs = refs[INNER_STEPS + 1], refs[INNER_STEPS + 2 : count]
    gram_ref, mix_a, mix_b, sums_ref = refs[count + NUM - INNER_STEPS - 1 :]
    par_y = lax.rem(lax.axis_index("gy"), 2)

    def corners(one, two):
        def read(slot):
            at = slice(8 * slot, 8 * slot + 8)
            return tuple(jnp.where(par_y == 0, one[n, at], two[n, at]) for n in range(2))

        return read

    place_pairs(
        lambda *at: jnp.where(par_y == 0, r2_ref[at], r1_ref[at]),
        lambda *at: jnp.where(par_y == 0, r1_ref[at], r2_ref[at]),
        corners(c2_ref, c1_ref), corners(c1_ref, c2_ref),
        1, 0, p_refs[0], d_ref, coef_refs, k_ref,
    )
    run_blocks(OUTER, p_refs, d_ref, coef_refs, split_kron(kron_ref), (mix_a, mix_b))

    sums_ref[...] = jnp.zeros_like(sums_ref)
    for lo_k, hi_k in ((0, 6), (6, NUM)):
        pairs = [(n, i, j) for n, (i, j) in enumerate(PAIRS) if lo_k <= j < hi_k]

        def body(r, accs, pairs=pairs, hi_k=hi_k):
            accs = list(accs)
            for c in range(2):
                for t in range(4):
                    vecs = [p_refs[k][RIM + r, 8 * c : 8 * c + 8, TILES[t]] for k in range(hi_k)]
                    for n, (_, i, j) in enumerate(pairs):
                        accs[n] = accs[n] + vecs[i] * vecs[j]
            return tuple(accs)

        accs = lax.fori_loop(0, ROWS // 2, body, tuple(jnp.zeros((8, 128), F32) for _ in pairs))
        for (n, _, _), acc in zip(pairs, accs):
            sums_ref[n : n + 1, :] = jnp.sum(acc, axis=0, keepdims=True)
    gram_ref[...] = lax.dot_general(
        jnp.ones((128, 128), F32), sums_ref[...], (((1,), (1,)), ((), ())),
        precision=lax.Precision.HIGHEST, preferred_element_type=F32,
    )


def small_solve(gram):
    inv = 1.0 / SCALE

    def total(values):
        values = list(values)
        while len(values) > 1:
            nxt = [values[k] + values[k + 1] for k in range(0, len(values) - 1, 2)]
            if len(values) % 2:
                nxt.append(values[-1])
            values = nxt
        return values[0]

    def shifted(vec):
        out = []
        for k in range(len(vec) + 1):
            terms = [vec[m] for m in (k - 1, k + 1) if 0 <= m < len(vec)]
            parts = [total(terms) * inv] if terms else []
            if k < len(vec):
                parts.append(vec[k] * CENTRE)
            out.append(total(parts))
        return out

    def dot(one, two):
        return total(x * y for x, y in zip(one, two))

    first = jnp.sqrt(gram[0][0] + GUARD)
    inv_first = 1.0 / first
    basis = [[inv_first]]
    images = [[gram[k][0] * inv_first for k in range(NUM)]]
    cosines, sines, upper = [], [], []
    target = [first]
    for col in range(ITERS):
        work = shifted(basis[col])
        image = [dot(work, gram[k]) for k in range(NUM)]
        coeffs = [dot(basis[i], image) for i in range(col + 1)]
        work = [
            total([work[k]] + [-(coeffs[i] * basis[i][k]) for i in range(col + 1) if k < len(basis[i])])
            for k in range(len(work))
        ]
        image = [total([image[k]] + [-(coeffs[i] * images[i][k]) for i in range(col + 1)]) for k in range(NUM)]
        subdiag = jnp.sqrt(jnp.maximum(dot(work, image), 0.0) + GUARD)
        if col + 1 < ITERS:
            scale = 1.0 / subdiag
            basis.append([x * scale for x in work])
            images.append([x * scale for x in image])
        column = list(coeffs)
        for k in range(col):
            a, b = column[k], column[k + 1]
            column[k] = cosines[k] * a + sines[k] * b
            column[k + 1] = cosines[k] * b - sines[k] * a
        a, b = column[col], subdiag
        radius = jnp.sqrt(a * a + b * b)
        inv_radius = 1.0 / radius
        cosines.append(a * inv_radius)
        sines.append(b * inv_radius)
        column[col] = radius
        upper.append((column, inv_radius))
        last = target[col]
        target[col] = cosines[col] * last
        target.append(-(sines[col] * last))
    weights = [None] * ITERS
    for col in reversed(range(ITERS)):
        rest = [target[col]] + [-(upper[k][0][col] * weights[k]) for k in range(col + 1, ITERS)]
        weights[col] = total(rest) * upper[col][1]
    coef = [total([weights[j] * basis[j][k] for j in range(k, ITERS)]) for k in range(ITERS)]
    return coef, shifted(coef)


def final_kernel(*refs):
    p_refs = refs[:NUM]
    rows_ref, x_ref, r_ref, xv_ref, rv_ref, work_ref, sem = refs[NUM:]
    summed = jnp.sum(rows_ref[...], axis=0, keepdims=True)
    gram = [[None] * NUM for _ in range(NUM)]
    for n, (i, j) in enumerate(PAIRS):
        gram[i][j] = gram[j][i] = jnp.broadcast_to(summed[:, n : n + 1], (8, 128))
    coef, image = small_solve(gram)
    for k in range(ITERS):
        work_ref[k] = coef[k]
    work_ref[ITERS] = 1.0 - image[0]
    for k in range(1, NUM):
        work_ref[ITERS + k] = -image[k]
    copies = []
    for b in range(ROWS // 8):
        rows = slice(8 * b, 8 * b + 8)
        for c in range(2):
            for t in range(2):
                upper = b >= 2
                first = HALF - 1 - 8 * (b - 2) - 7 if upper else RIM + 8 * b
                tile = TILES[2 + t] if upper else TILES[t]
                xs = rs = None
                for k in range(NUM):
                    vec = p_refs[k][first : first + 8, 8 * c : 8 * c + 8, tile]
                    part = vec * work_ref[ITERS + k]
                    rs = part if rs is None else rs + part
                    if k < ITERS:
                        part = vec * work_ref[k]
                        xs = part if xs is None else xs + part
                where = (slice(8 * c, 8 * c + 8), rows, slice(128 * t, 128 * t + 128))
                for ref, value in ((xv_ref, xs), (rv_ref, rs)):
                    if upper:
                        value = jnp.stack([pltpu.roll(value[7 - i], 64, 1) for i in range(8)])
                    ref[where] = jnp.swapaxes(value, 0, 1)
        for n, (src, dst) in enumerate(((xv_ref, x_ref), (rv_ref, r_ref))):
            copy = pltpu.make_async_copy(src.at[:, rows], dst.at[:, rows], sem.at[2 * b + n])
            copy.start()
            copies.append(copy)
    for copy in copies:
        copy.wait()


def diffusion_table(lat_total):
    row = np.arange(-RIM, lat_total + RIM, dtype=np.float64)
    phi = -math.pi / 2 + (row + 0.5) * (math.pi / lat_total)
    kx = DIFF_LON / (np.cos(phi) ** 2 + 0.1)
    kx = np.where((row >= 0) & (row < lat_total), kx, 0.0)
    return np.repeat(kx[:, None], 128, axis=1).astype(np.float32)


VMEM = pl.BlockSpec(memory_space=pltpu.VMEM)
HBM = pl.BlockSpec(memory_space=pltpu.HBM)


def shape(*dims):
    return jax.ShapeDtypeStruct(dims, F32)


def pairing(count, odd, closed):
    pairs = []
    for i in range(count):
        partner = i + 1 if (i % 2 == 0) != odd else i - 1
        if closed:
            partner %= count
        if 0 <= partner < count:
            pairs.append((i, partner))
    return pairs


def per_device(forcing, damping, coupling, wind_lon, wind_lat, *, nx, ny):
    inputs = (forcing, damping, wind_lon, wind_lat, coupling, jnp.asarray(diffusion_table(ny * ROWS)))
    s1, s2, x1, x2, couple, k_rows = pl.pallas_call(
        pack_kernel,
        in_specs=[HBM] * 6,
        out_specs=[VMEM] * 6,
        out_shape=[shape(34, 16, COLS)] * 2
        + [shape(2, 72, 128)] * 2
        + [shape(CH, CH), shape(EXT_ROWS, 128)],
        scratch_shapes=[
            pltpu.VMEM((CH, ROWS, COLS), F32),
            pltpu.VMEM((CH, ROWS, COLS), F32),
            pltpu.VMEM((ROWS, COLS), F32),
            pltpu.VMEM((ROWS, COLS), F32),
            pltpu.SemaphoreType.DMA((6,)),
        ],
        compiler_params=pltpu.CompilerParams(vmem_limit_bytes=8 * 2**20),
        name="pack",
    )(*(pltpu.with_memory_space_constraint(x, pltpu.HBM) for x in inputs))
    r1 = lax.ppermute(s1, "gy", pairing(ny, False, False))
    r2 = lax.ppermute(s2, "gy", pairing(ny, True, False))
    g1 = lax.ppermute(x1, "gx", pairing(nx, False, True))
    g2 = lax.ppermute(x2, "gx", pairing(nx, True, True))
    k1, k2 = pl.pallas_call(
        corner_kernel,
        in_specs=[VMEM] * 2,
        out_specs=[VMEM] * 2,
        out_shape=[shape(2, 72, 128)] * 2,
        compiler_params=pltpu.CompilerParams(vmem_limit_bytes=2**20),
        name="corner",
    )(g1, g2)
    c1 = lax.ppermute(k1, "gy", pairing(ny, False, False))
    c2 = lax.ppermute(k2, "gy", pairing(ny, True, False))
    field = shape(HALF + GHOST + 1, CH, WIDE)
    mix = [pltpu.VMEM((8, CH, WIDE), F32), pltpu.VMEM((9, CH, WIDE), F32)]
    carried = [field] * (INNER_STEPS + 1) + [shape(HALF, CH, WIDE)]
    carried += [shape(6, HALF, COLS)] * 2 + [shape(6, HALF, 128)]
    first = [carried[n] for n in (0, -4, -3, -2)]
    stage = pl.pallas_call(
        stage_kernel,
        in_specs=[VMEM] * 4,
        out_specs=[VMEM] * 5,
        out_shape=first + [shape(8 * CH, 8 * CH)],
        compiler_params=pltpu.CompilerParams(vmem_limit_bytes=4 * 2**20),
        cost_estimate=pl.CostEstimate(flops=10**7, bytes_accessed=2**20, transcendentals=0),
        name="stage",
    )
    *staged, kron = stage(s1, s2, couple, k_rows)
    where = (0, INNER_STEPS + 1, INNER_STEPS + 2, INNER_STEPS + 3)
    state = pl.pallas_call(
        inner_kernel,
        in_specs=[VMEM] * 8,
        out_specs=[VMEM] * len(carried),
        out_shape=carried,
        input_output_aliases={4 + n: at for n, at in enumerate(where)},
        scratch_shapes=mix,
        compiler_params=pltpu.CompilerParams(vmem_limit_bytes=8 * 2**20),
        cost_estimate=pl.CostEstimate(flops=10**8, bytes_accessed=2**20, transcendentals=0),
        name="inner",
    )(g1, g2, k_rows, kron, *staged)
    extra = [field] * (NUM - INNER_STEPS - 1)
    results = pl.pallas_call(
        outer_kernel,
        in_specs=[VMEM] * (6 + len(carried)),
        out_specs=[VMEM] * (len(carried) + len(extra) + 1),
        out_shape=carried + extra + [shape(128, 128)],
        input_output_aliases={6 + n: n for n in range(len(carried))},
        scratch_shapes=mix + [pltpu.VMEM((128, 128), F32)],
        compiler_params=pltpu.CompilerParams(vmem_limit_bytes=8 * 2**20),
        name="outer",
    )(r1, r2, c1, c2, k_rows, kron, *state)
    basis = results[: INNER_STEPS + 1] + results[len(carried) : -1]
    rows = lax.all_to_all(results[-1], ("gx", "gy"), 0, 0, tiled=True)
    return pl.pallas_call(
        final_kernel,
        in_specs=[VMEM] * (NUM + 1),
        out_specs=[HBM, HBM],
        out_shape=[shape(CH, ROWS, COLS)] * 2,
        scratch_shapes=[
            pltpu.VMEM((CH, ROWS, COLS), F32),
            pltpu.VMEM((CH, ROWS, COLS), F32),
            pltpu.VMEM((ITERS + NUM, 8, 128), F32),
            pltpu.SemaphoreType.DMA((ROWS // 4,)),
        ],
        compiler_params=pltpu.CompilerParams(vmem_limit_bytes=8 * 2**20),
        name="finish",
    )(*basis, rows)


def solution(mesh):
    spec = P(None, "gy", "gx")
    flat = P("gy", "gx")
    return jax.shard_map(
        functools.partial(per_device, nx=mesh.shape["gx"], ny=mesh.shape["gy"]),
        mesh=mesh,
        in_specs=(spec, spec, P(), flat, flat),
        out_specs=(spec, spec),
        check_vma=False,
    )
```

```python
import functools
import math

import jax
import jax.numpy as jnp
import numpy as np
from jax import lax
from jax.experimental import pallas as pl
from jax.experimental.pallas import tpu as pltpu
from jax.sharding import PartitionSpec as P


ITERS = 8
CH = 16
ROWS = 32
COLS = 256
RIM = 2 * ITERS
EXT_ROWS = ROWS + 2 * RIM
COUPLE = 0.25
DIFF_LAT = 0.5
DIFF_LON = 0.5
GUARD = 1.0

LOW, HIGH = 1.5, 26.0
CENTRE = (LOW + HIGH) / 2
SCALE = 4.0 / (HIGH - LOW)
NUM = ITERS + 1
PAIRS = [(i, j) for j in range(NUM) for i in range(j + 1)]
F32 = jnp.float32


def own_row(ref, rest, half, row, *at):
    first = 2 * half
    if row < 16:
        return ref[(row, *at)]
    if row >= 32:
        return ref[(row - 2, *at)]
    row -= 16
    if first <= row < first + 14:
        return ref[(16 + row - first, *at)]
    return rest[(row % 14, *at)]


def pack_kernel(
    f_hbm, d_hbm, wl_hbm, wt_hbm, cp_hbm, tab_hbm,
    s1_ref, s2_ref, x1_ref, x2_ref, cp_ref, k_ref, rest_ref,
    f_ref, d_ref, wl_ref, wt_ref, sem,
):
    start = pl.multiple_of(lax.axis_index("gy") * ROWS, ROWS)
    copies = [
        pltpu.make_async_copy(src, dst, sem.at[n])
        for n, (src, dst) in enumerate(
            (
                (f_hbm, f_ref), (d_hbm, d_ref), (wl_hbm, wl_ref), (wt_hbm, wt_ref),
                (cp_hbm, cp_ref), (tab_hbm.at[pl.ds(start, EXT_ROWS)], k_ref),
            )
        )
    ]
    for copy in copies:
        copy.start()
    for copy in copies:
        copy.wait()
    par_y = lax.rem(lax.axis_index("gy"), 2)
    par_x = lax.rem(lax.axis_index("gx"), 2)
    for n, (ref, half) in enumerate(((s1_ref, 1 - par_y), (s2_ref, par_y))):
        offs = [pl.multiple_of(half * 16 + 8 * q, 8) for q in range(2)]
        for c in range(2):
            subs = slice(8 * c, 8 * c + 8)
            rows = [jnp.swapaxes(d_ref[subs, pl.ds(off, 8), :], 0, 1) for off in offs]
            for q in range(2):
                ref[pl.ds(16 + 8 * q - 2 * half, 8), subs, :] = rows[q]
            rest_ref[n, :, subs, :] = jnp.where(half == 1, rows[0][:2], rows[1][6:])
            for q in range(2):
                ref[8 * q : 8 * q + 8, subs, :] = jnp.swapaxes(f_ref[subs, pl.ds(offs[q], 8), :], 0, 1)
        off = pl.multiple_of(half * 16, 16)
        ref[30] = wl_ref[pl.ds(off, 16), :]
        ref[31] = wt_ref[pl.ds(off, 16), :]
    group = lax.broadcasted_iota(jnp.int32, (8, 128), 1) // 16

    def gather(tiles):
        left = jnp.zeros((8, 128), F32)
        right = jnp.zeros((8, 128), F32)
        for g, (low, high) in enumerate(tiles):
            left = jnp.where(group == g, pltpu.roll(low, 16 * g, 1) if g else low, left)
            shift = (16 * g + 16) % 128
            right = jnp.where(group == g, pltpu.roll(high, shift, 1) if shift else high, right)
        return jnp.where(par_x == 0, right, left), jnp.where(par_x == 0, left, right)

    winds = gather(
        [
            (ref[8 * q : 8 * q + 8, :128], ref[8 * q : 8 * q + 8, 128:])
            for ref in (wl_ref, wt_ref)
            for q in range(4)
        ]
    )
    for half in range(2):
        slot = 0
        for base in (0, 16):
            for q in range(2):
                for c in range(2):
                    tiles = []
                    for g in range(8):
                        row = base + 8 * q + g
                        pick = []
                        for t in range(2):
                            at = (slice(8 * c, 8 * c + 8), slice(128 * t, 128 * t + 128))
                            one = own_row(s1_ref, rest_ref.at[0], half, row, *at)
                            two = own_row(s2_ref, rest_ref.at[1], half, row, *at)
                            pick.append(jnp.where(par_y == half, two, one))
                        tiles.append(tuple(pick))
                    first, second = gather(tiles)
                    x1_ref[half, 8 * slot : 8 * slot + 8, :] = first
                    x2_ref[half, 8 * slot : 8 * slot + 8, :] = second
                    slot += 1
        x1_ref[half, 64:72, :] = winds[0]
        x2_ref[half, 64:72, :] = winds[1]


HALF = EXT_ROWS // 2
GHOST = 2
WIDE = 2 * COLS + 128
TILES = [slice(128 * t, 128 * t + 128) for t in range(5)]


def place_pairs(
    low, high, low_sides, high_sides, low_half, base, p0_ref, d_ref, coef_refs, k_ref, main=True, edge=True
):
    par_x = lax.rem(lax.axis_index("gx"), 2)
    lane = lax.broadcasted_iota(jnp.int32, (8, 128), 1)
    turned = jnp.logical_and(lane >= 48, lane < 80)
    coef_low, coef_high, coef_edge = coef_refs
    spans = [t for t in range(3) if (edge if t == 2 else main)]

    def turn(x, by):
        return pltpu.roll(x, by % 128, 1) if by % 128 else x

    def sides(reader, slot):
        a, b = reader(slot)
        return jnp.where(par_x == 0, a, b), jnp.where(par_x == 0, b, a)

    def spread(low_pair, low_group, high_pair, high_group):
        out = jnp.where(lane < 16, turn(low_pair[0], -16 * low_group), 0.0)
        out = jnp.where(lane >= 112, turn(low_pair[1], 112 - 16 * low_group), out)
        upper = jnp.where(lane >= 64, turn(high_pair[0], 64 - 16 * high_group), turn(high_pair[1], 48 - 16 * high_group))
        return jnp.where(turned, upper, out)

    scales = {}
    edges = {}
    wind_sides = (sides(low_sides, 8), sides(high_sides, 8)) if edge else None
    for side, (reader, half, sign, first) in enumerate(
        ((low, low_half, 1.0, base), (high, 1 - low_half, -1.0, EXT_ROWS - base - 16))
    ):
        for q in range(2):
            k = k_ref[first + 8 * q : first + 8 * q + 8]
            live = jnp.where(k > 0.0, 1.0, 0.0)
            kx = k * SCALE
            half_lat = live * (SCALE * DIFF_LAT)
            scales[side, q] = (live * SCALE, live * (SCALE * (1.0 + 2.0 * DIFF_LAT - CENTRE)) + 2.0 * kx)
            for t in spans:
                winds = []
                for field in range(2):
                    if t < 2:
                        wind = reader(32 + field, slice(8 * q, 8 * q + 8), TILES[t])
                        if side:
                            wind = turn(wind, 64)
                    else:
                        group = 4 * field + 2 * half + q
                        east, west = wind_sides[side]
                        if side:
                            wind = jnp.where(lane >= 64, turn(east, 64 - 16 * group), turn(west, 48 - 16 * group))
                        else:
                            wind = jnp.where(lane < 64, turn(east, -16 * group), turn(west, 112 - 16 * group))
                    winds.append(wind * (live * (SCALE / 12.0)))
                lon, lat = winds[0], winds[1] * sign
                values = (
                    8.0 * lon - kx, -8.0 * lon - kx, -lon,
                    8.0 * lat - half_lat, -8.0 * lat - half_lat, -lat,
                )
                for n, value in enumerate(values):
                    if t == 2:
                        edges[side, q, n] = value
                    elif side:
                        row = first - HALF + 8 * q
                        coef_high[n, row : row + 8, TILES[t]] = value
                    else:
                        coef_low[n, first + 8 * q : first + 8 * q + 8, TILES[t]] = value
    inside = jnp.logical_or(lane < 16, lane >= 112)[:1]
    turned_row = turned[:1]
    for i in range(16):
        u = base + i
        j = 15 - i
        for n in range(6 if edge else 0):
            a = edges[0, i // 8, n][i % 8 : i % 8 + 1]
            b = edges[1, j // 8, n][j % 8 : j % 8 + 1]
            coef_edge[n, u : u + 1, :] = jnp.where(turned_row, b, jnp.where(inside, a, 0.0))
    for c in range(2):
        subs = slice(8 * c, 8 * c + 8)
        pairs = {}
        for kind in range(2 if edge else 0):
            for q in range(2):
                pairs[kind, 0, q] = sides(low_sides, 4 * kind + 2 * q + c)
                pairs[kind, 1, q] = sides(high_sides, 4 * kind + 2 * q + c)
        for i in range(16):
            u = base + i
            j = 15 - i
            mul_l, add_l = (x[i % 8 : i % 8 + 1] for x in scales[0, i // 8])
            mul_h, add_h = (x[j % 8 : j % 8 + 1] for x in scales[1, j // 8])
            for t in range(2 if main else 0):
                p0_ref[u, subs, TILES[t]] = low(i, subs, TILES[t])
                p0_ref[u, subs, TILES[2 + t]] = turn(high(j, subs, TILES[t]), 64)
                if u < 2:
                    continue
                d_ref[u, subs, TILES[t]] = low(16 + i, subs, TILES[t]) * mul_l + add_l
                d_ref[u, subs, TILES[2 + t]] = turn(high(16 + j, subs, TILES[t]), 64) * mul_h + add_h
            if not edge:
                continue
            f_edge, d_edge = (
                spread(pairs[kind, 0, i // 8], i % 8, pairs[kind, 1, j // 8], j % 8) for kind in range(2)
            )
            p0_ref[u, subs, TILES[4]] = f_edge
            if u < 2:
                continue
            mul = jnp.where(turned_row, mul_h, mul_l)
            add = jnp.where(turned_row, add_h, add_l)
            d_ref[u, subs, TILES[4]] = d_edge * mul + add


def mirror(p_ref):
    for g in range(GHOST):
        for dst, src in zip((0, 1, 2, 3, 4), (2, 3, 0, 1, 4)):
            p_ref[HALF + g, :, TILES[dst]] = pltpu.roll(p_ref[HALF - 1 - g, :, TILES[src]], 64, 1)


def split_kron(kron_ref):
    kron = kron_ref[...]
    hi = kron.astype(jnp.bfloat16)
    return hi, (kron - hi.astype(F32)).astype(jnp.bfloat16)


def run_blocks(blocks, p_refs, d_ref, coef_refs, kron, mix_refs):
    lane = lax.broadcasted_iota(jnp.int32, (8, 128), 1)
    coef_low, coef_high, coef_edge = coef_refs

    def width(step):
        return WIDE if step < ITERS else 2 * COLS

    def mix(index):
        step, u0, count = blocks[index]
        size = count * CH
        kron_hi, kron_lo = (k[:size, :size] for k in kron)
        flat = p_refs[step - 1][u0 : u0 + count, :, : width(step)].reshape(size, width(step))
        hi = flat.astype(jnp.bfloat16)
        lo = (flat - hi.astype(F32)).astype(jnp.bfloat16)
        mixed = jnp.dot(kron_hi, hi, preferred_element_type=F32)
        mixed = mixed + jnp.dot(kron_hi, lo, preferred_element_type=F32)
        mixed = mixed + jnp.dot(kron_lo, hi, preferred_element_type=F32)
        mix_refs[index % 2][:count, :, : width(step)] = mixed.reshape(count, CH, width(step))

    def shifted(tiles, by):
        rolled = [pltpu.roll(x, by % 128, 1) for x in tiles]
        if by < 0:
            low, high = lane >= 128 + by, jnp.logical_and(lane >= 64 + by, lane < 64)
            nexts = (1, 4, 3, 4)
        else:
            low, high = lane < by, jnp.logical_and(lane >= 64, lane < 64 + by)
            nexts = (4, 0, 4, 2)
        ends = (0, 2) if by < 0 else (1, 3)
        out = [jnp.where(low if t < 2 else high, rolled[nexts[t]], rolled[t]) for t in range(4)]
        out.append(jnp.where(low, rolled[ends[0]], jnp.where(high, rolled[ends[1]], rolled[4])))
        return out

    mix(0)
    for index, (step, u0, count) in enumerate(blocks):
        more = index + 1 < len(blocks)
        late = False
        if more:
            step_n, u_n, count_n = blocks[index + 1]
            late = step_n == step + 1 and u_n < u0 + count and u0 < u_n + count_n
        if more and not late:
            mix(index + 1)
        src, dst = p_refs[step - 1], p_refs[step]
        for i, s in [(i, s) for i in range(count) for s in (slice(0, 8), slice(8, 16))]:
            u = u0 + i
            centre = [src[u, s, t] for t in TILES]
            east, west = shifted(centre, -1), shifted(centre, 1)
            east2, west2 = shifted(centre, -2), shifted(centre, 2)
            span = range(width(step) // 128)

            def coef(n):
                out = []
                for t in span:
                    if t < 2:
                        out.append(coef_low[n, u : u + 1, TILES[t]])
                    elif t < 4:
                        v = HALF - 1 - u
                        out.append(coef_high[n, v : v + 1, TILES[t - 2]])
                    else:
                        out.append(coef_edge[n, u : u + 1, :])
                return out

            acc = [mix_refs[index % 2][i, s, TILES[t]] + d_ref[u, s, TILES[t]] * centre[t] for t in span]
            if step > 1:
                acc = [acc[t] - p_refs[step - 2][u, s, TILES[t]] for t in span]
            for n, values in (
                (0, lambda t: east[t]),
                (1, lambda t: west[t]),
                (2, lambda t: east2[t] - west2[t]),
                (3, lambda t: src[u + 1, s, TILES[t]]),
                (4, lambda t: src[u - 1, s, TILES[t]]),
                (5, lambda t: src[u + 2, s, TILES[t]] - src[u - 2, s, TILES[t]]),
            ):
                scale = coef(n)
                acc = [acc[t] + scale[t] * values(t) for t in span]
            for t in span:
                dst[u, s, TILES[t]] = acc[t]
        if u0 + count == HALF and step < ITERS:
            mirror(dst)
        if late:
            mix(index + 1)


INNER_STEPS = 6
INNER = []
OUTER = []
for _j in range(1, NUM):
    _edge = RIM + 2 * _j
    if _j <= INNER_STEPS:
        _rest = HALF - _edge
        if _rest > 8:
            INNER.append((_j, _edge + 8, _rest - 8))
        INNER.append((_j, _edge, min(_rest, 8)))
        OUTER += [(_j, 2 * _j + 8, 8), (_j, 2 * _j, 8)]
    elif _j < ITERS:
        OUTER += [(_j, 26, 6), (_j, 20, 6), (_j, 14, 6)]
    else:
        OUTER += [(_j, 24, 8), (_j, 16, 8)]


def corner_kernel(g1_ref, g2_ref, k1_ref, k2_ref):
    par_y = lax.rem(lax.axis_index("gy"), 2)
    for n, g_ref in enumerate((g1_ref, g2_ref)):
        k1_ref[n] = g_ref[1 - par_y]
        k2_ref[n] = g_ref[par_y]


def stage_kernel(s1_ref, s2_ref, cp_ref, k_ref, rest_ref, p0_ref, d_ref, coef_low, coef_high, kron_ref):
    par_y = lax.rem(lax.axis_index("gy"), 2)
    size = 8 * CH
    pick = lax.broadcasted_iota(jnp.int32, (size, CH), 0) % CH
    pick = (pick == lax.broadcasted_iota(jnp.int32, (size, CH), 1)).astype(F32)
    tall = jnp.dot(
        pick, cp_ref[...] * (COUPLE * SCALE), precision=lax.Precision.HIGHEST, preferred_element_type=F32
    )
    full = lax.dot_general(
        tall, pick, (((1,), (1,)), ((), ())), precision=lax.Precision.HIGHEST, preferred_element_type=F32
    )
    row = lax.broadcasted_iota(jnp.int32, (size, size), 0) // CH
    col = lax.broadcasted_iota(jnp.int32, (size, size), 1) // CH
    kron_ref[...] = jnp.where(row == col, full, 0.0)
    place_pairs(
        lambda *at: jnp.where(
            par_y == 0, own_row(s2_ref, rest_ref.at[1], 0, *at), own_row(s1_ref, rest_ref.at[0], 0, *at)
        ),
        lambda *at: jnp.where(
            par_y == 0, own_row(s1_ref, rest_ref.at[0], 1, *at), own_row(s2_ref, rest_ref.at[1], 1, *at)
        ),
        None, None, 0, RIM, p0_ref, d_ref, (coef_low, coef_high, None), k_ref, edge=False,
    )


def inner_kernel(g1_ref, g2_ref, k_ref, kron_ref, *refs):
    refs = refs[4:]
    p_refs = refs[: INNER_STEPS + 1]
    d_ref, *coef_refs = refs[INNER_STEPS + 1 : INNER_STEPS + 5]
    mix_refs = refs[INNER_STEPS + 5 :]
    place_pairs(
        None, None,
        lambda slot: (g1_ref[0, 8 * slot : 8 * slot + 8], g2_ref[0, 8 * slot : 8 * slot + 8]),
        lambda slot: (g1_ref[1, 8 * slot : 8 * slot + 8], g2_ref[1, 8 * slot : 8 * slot + 8]),
        0, RIM, p_refs[0], d_ref, coef_refs, k_ref, main=False,
    )
    mirror(p_refs[0])
    run_blocks(INNER, p_refs, d_ref, coef_refs, split_kron(kron_ref), mix_refs)


def outer_kernel(r1_ref, r2_ref, c1_ref, c2_ref, k_ref, kron_ref, *refs):
    count = INNER_STEPS + 5
    refs = refs[count:]
    p_refs = refs[: INNER_STEPS + 1] + refs[count : count + NUM - INNER_STEPS - 1]
    d_ref, coef_refs = refs[INNER_STEPS + 1], refs[INNER_STEPS + 2 : count]
    gram_ref, mix_a, mix_b, sums_ref = refs[count + NUM - INNER_STEPS - 1 :]
    par_y = lax.rem(lax.axis_index("gy"), 2)

    def corners(one, two):
        def read(slot):
            at = slice(8 * slot, 8 * slot + 8)
            return tuple(jnp.where(par_y == 0, one[n, at], two[n, at]) for n in range(2))

        return read

    place_pairs(
        lambda *at: jnp.where(par_y == 0, own_row(r2_ref, None, 1, *at), own_row(r1_ref, None, 1, *at)),
        lambda *at: jnp.where(par_y == 0, own_row(r1_ref, None, 0, *at), own_row(r2_ref, None, 0, *at)),
        corners(c2_ref, c1_ref), corners(c1_ref, c2_ref),
        1, 0, p_refs[0], d_ref, coef_refs, k_ref,
    )
    run_blocks(OUTER, p_refs, d_ref, coef_refs, split_kron(kron_ref), (mix_a, mix_b))

    sums_ref[...] = jnp.zeros_like(sums_ref)
    for lo_k, hi_k in ((0, 6), (6, NUM)):
        pairs = [(n, i, j) for n, (i, j) in enumerate(PAIRS) if lo_k <= j < hi_k]

        def body(r, accs, pairs=pairs, hi_k=hi_k):
            accs = list(accs)
            for c in range(2):
                for t in range(4):
                    vecs = [p_refs[k][RIM + r, 8 * c : 8 * c + 8, TILES[t]] for k in range(hi_k)]
                    for n, (_, i, j) in enumerate(pairs):
                        accs[n] = accs[n] + vecs[i] * vecs[j]
            return tuple(accs)

        accs = lax.fori_loop(0, ROWS // 2, body, tuple(jnp.zeros((8, 128), F32) for _ in pairs))
        for (n, _, _), acc in zip(pairs, accs):
            sums_ref[n : n + 1, :] = jnp.sum(acc, axis=0, keepdims=True)
    gram_ref[...] = lax.dot_general(
        jnp.ones((128, 128), F32), sums_ref[...], (((1,), (1,)), ((), ())),
        precision=lax.Precision.HIGHEST, preferred_element_type=F32,
    )


def small_solve(gram):
    inv = 1.0 / SCALE

    def total(values):
        values = list(values)
        while len(values) > 1:
            nxt = [values[k] + values[k + 1] for k in range(0, len(values) - 1, 2)]
            if len(values) % 2:
                nxt.append(values[-1])
            values = nxt
        return values[0]

    def shifted(vec):
        out = []
        for k in range(len(vec) + 1):
            terms = [vec[m] for m in (k - 1, k + 1) if 0 <= m < len(vec)]
            parts = [total(terms) * inv] if terms else []
            if k < len(vec):
                parts.append(vec[k] * CENTRE)
            out.append(total(parts))
        return out

    def dot(one, two):
        return total(x * y for x, y in zip(one, two))

    first = jnp.sqrt(gram[0][0] + GUARD)
    inv_first = 1.0 / first
    basis = [[inv_first]]
    images = [[gram[k][0] * inv_first for k in range(NUM)]]
    cosines, sines, upper = [], [], []
    target = [first]
    for col in range(ITERS):
        work = shifted(basis[col])
        image = [dot(work, gram[k]) for k in range(NUM)]
        coeffs = [dot(basis[i], image) for i in range(col + 1)]
        work = [
            total([work[k]] + [-(coeffs[i] * basis[i][k]) for i in range(col + 1) if k < len(basis[i])])
            for k in range(len(work))
        ]
        image = [total([image[k]] + [-(coeffs[i] * images[i][k]) for i in range(col + 1)]) for k in range(NUM)]
        subdiag = jnp.sqrt(jnp.maximum(dot(work, image), 0.0) + GUARD)
        if col + 1 < ITERS:
            scale = 1.0 / subdiag
            basis.append([x * scale for x in work])
            images.append([x * scale for x in image])
        column = list(coeffs)
        for k in range(col):
            a, b = column[k], column[k + 1]
            column[k] = cosines[k] * a + sines[k] * b
            column[k + 1] = cosines[k] * b - sines[k] * a
        a, b = column[col], subdiag
        radius = jnp.sqrt(a * a + b * b)
        inv_radius = 1.0 / radius
        cosines.append(a * inv_radius)
        sines.append(b * inv_radius)
        column[col] = radius
        upper.append((column, inv_radius))
        last = target[col]
        target[col] = cosines[col] * last
        target.append(-(sines[col] * last))
    weights = [None] * ITERS
    for col in reversed(range(ITERS)):
        rest = [target[col]] + [-(upper[k][0][col] * weights[k]) for k in range(col + 1, ITERS)]
        weights[col] = total(rest) * upper[col][1]
    coef = [total([weights[j] * basis[j][k] for j in range(k, ITERS)]) for k in range(ITERS)]
    return coef, shifted(coef)


def final_kernel(*refs):
    p_refs = refs[:NUM]
    rows_ref, x_ref, r_ref, xv_ref, rv_ref, work_ref, sem = refs[NUM:]
    summed = jnp.sum(rows_ref[...], axis=0, keepdims=True)
    gram = [[None] * NUM for _ in range(NUM)]
    for n, (i, j) in enumerate(PAIRS):
        gram[i][j] = gram[j][i] = jnp.broadcast_to(summed[:, n : n + 1], (8, 128))
    coef, image = small_solve(gram)
    for k in range(ITERS):
        work_ref[k] = coef[k]
    work_ref[ITERS] = 1.0 - image[0]
    for k in range(1, NUM):
        work_ref[ITERS + k] = -image[k]
    copies = []
    for b in range(ROWS // 8):
        rows = slice(8 * b, 8 * b + 8)
        for c in range(2):
            for t in range(2):
                upper = b >= 2
                first = HALF - 1 - 8 * (b - 2) - 7 if upper else RIM + 8 * b
                tile = TILES[2 + t] if upper else TILES[t]
                xs = rs = None
                for k in range(NUM):
                    vec = p_refs[k][first : first + 8, 8 * c : 8 * c + 8, tile]
                    part = vec * work_ref[ITERS + k]
                    rs = part if rs is None else rs + part
                    if k < ITERS:
                        part = vec * work_ref[k]
                        xs = part if xs is None else xs + part
                where = (slice(8 * c, 8 * c + 8), rows, slice(128 * t, 128 * t + 128))
                for ref, value in ((xv_ref, xs), (rv_ref, rs)):
                    if upper:
                        value = jnp.stack([pltpu.roll(value[7 - i], 64, 1) for i in range(8)])
                    ref[where] = jnp.swapaxes(value, 0, 1)
        for n, (src, dst) in enumerate(((xv_ref, x_ref), (rv_ref, r_ref))):
            copy = pltpu.make_async_copy(src.at[:, rows], dst.at[:, rows], sem.at[2 * b + n])
            copy.start()
            copies.append(copy)
    for copy in copies:
        copy.wait()


def diffusion_table(lat_total):
    row = np.arange(-RIM, lat_total + RIM, dtype=np.float64)
    phi = -math.pi / 2 + (row + 0.5) * (math.pi / lat_total)
    kx = DIFF_LON / (np.cos(phi) ** 2 + 0.1)
    kx = np.where((row >= 0) & (row < lat_total), kx, 0.0)
    return np.repeat(kx[:, None], 128, axis=1).astype(np.float32)


VMEM = pl.BlockSpec(memory_space=pltpu.VMEM)
HBM = pl.BlockSpec(memory_space=pltpu.HBM)


def shape(*dims):
    return jax.ShapeDtypeStruct(dims, F32)


def pairing(count, odd, closed):
    pairs = []
    for i in range(count):
        partner = i + 1 if (i % 2 == 0) != odd else i - 1
        if closed:
            partner %= count
        if 0 <= partner < count:
            pairs.append((i, partner))
    return pairs


def per_device(forcing, damping, coupling, wind_lon, wind_lat, *, nx, ny):
    inputs = (forcing, damping, wind_lon, wind_lat, coupling, jnp.asarray(diffusion_table(ny * ROWS)))
    s1, s2, x1, x2, couple, k_rows, rest = pl.pallas_call(
        pack_kernel,
        in_specs=[HBM] * 6,
        out_specs=[VMEM] * 7,
        out_shape=[shape(32, 16, COLS)] * 2
        + [shape(2, 72, 128)] * 2
        + [shape(CH, CH), shape(EXT_ROWS, 128), shape(2, 2, CH, COLS)],
        scratch_shapes=[
            pltpu.VMEM((CH, ROWS, COLS), F32),
            pltpu.VMEM((CH, ROWS, COLS), F32),
            pltpu.VMEM((ROWS, COLS), F32),
            pltpu.VMEM((ROWS, COLS), F32),
            pltpu.SemaphoreType.DMA((6,)),
        ],
        compiler_params=pltpu.CompilerParams(vmem_limit_bytes=8 * 2**20),
        name="pack",
    )(*(pltpu.with_memory_space_constraint(x, pltpu.HBM) for x in inputs))
    r1 = lax.ppermute(s1, "gy", pairing(ny, False, False))
    r2 = lax.ppermute(s2, "gy", pairing(ny, True, False))
    g1 = lax.ppermute(x1, "gx", pairing(nx, False, True))
    g2 = lax.ppermute(x2, "gx", pairing(nx, True, True))
    k1, k2 = pl.pallas_call(
        corner_kernel,
        in_specs=[VMEM] * 2,
        out_specs=[VMEM] * 2,
        out_shape=[shape(2, 72, 128)] * 2,
        compiler_params=pltpu.CompilerParams(vmem_limit_bytes=2**20),
        name="corner",
    )(g1, g2)
    c1 = lax.ppermute(k1, "gy", pairing(ny, False, False))
    c2 = lax.ppermute(k2, "gy", pairing(ny, True, False))
    field = shape(HALF + GHOST + 1, CH, WIDE)
    mix = [pltpu.VMEM((8, CH, WIDE), F32), pltpu.VMEM((9, CH, WIDE), F32)]
    carried = [field] * (INNER_STEPS + 1) + [shape(HALF, CH, WIDE)]
    carried += [shape(6, HALF, COLS)] * 2 + [shape(6, HALF, 128)]
    first = [carried[n] for n in (0, -4, -3, -2)]
    stage = pl.pallas_call(
        stage_kernel,
        in_specs=[VMEM] * 5,
        out_specs=[VMEM] * 5,
        out_shape=first + [shape(8 * CH, 8 * CH)],
        compiler_params=pltpu.CompilerParams(vmem_limit_bytes=4 * 2**20),
        cost_estimate=pl.CostEstimate(flops=10**7, bytes_accessed=2**20, transcendentals=0),
        name="stage",
    )
    *staged, kron = stage(s1, s2, couple, k_rows, rest)
    where = (0, INNER_STEPS + 1, INNER_STEPS + 2, INNER_STEPS + 3)
    state = pl.pallas_call(
        inner_kernel,
        in_specs=[VMEM] * 8,
        out_specs=[VMEM] * len(carried),
        out_shape=carried,
        input_output_aliases={4 + n: at for n, at in enumerate(where)},
        scratch_shapes=mix,
        compiler_params=pltpu.CompilerParams(vmem_limit_bytes=8 * 2**20),
        cost_estimate=pl.CostEstimate(flops=10**8, bytes_accessed=2**20, transcendentals=0),
        name="inner",
    )(g1, g2, k_rows, kron, *staged)
    extra = [field] * (NUM - INNER_STEPS - 1)
    results = pl.pallas_call(
        outer_kernel,
        in_specs=[VMEM] * (6 + len(carried)),
        out_specs=[VMEM] * (len(carried) + len(extra) + 1),
        out_shape=carried + extra + [shape(128, 128)],
        input_output_aliases={6 + n: n for n in range(len(carried))},
        scratch_shapes=mix + [pltpu.VMEM((128, 128), F32)],
        compiler_params=pltpu.CompilerParams(vmem_limit_bytes=8 * 2**20),
        name="outer",
    )(r1, r2, c1, c2, k_rows, kron, *state)
    basis = results[: INNER_STEPS + 1] + results[len(carried) : -1]
    rows = lax.all_to_all(results[-1], ("gx", "gy"), 0, 0, tiled=True)
    return pl.pallas_call(
        final_kernel,
        in_specs=[VMEM] * (NUM + 1),
        out_specs=[HBM, HBM],
        out_shape=[shape(CH, ROWS, COLS)] * 2,
        scratch_shapes=[
            pltpu.VMEM((CH, ROWS, COLS), F32),
            pltpu.VMEM((CH, ROWS, COLS), F32),
            pltpu.VMEM((ITERS + NUM, 8, 128), F32),
            pltpu.SemaphoreType.DMA((ROWS // 4,)),
        ],
        compiler_params=pltpu.CompilerParams(vmem_limit_bytes=8 * 2**20),
        name="finish",
    )(*basis, rows)


def solution(mesh):
    spec = P(None, "gy", "gx")
    flat = P("gy", "gx")
    return jax.shard_map(
        functools.partial(per_device, nx=mesh.shape["gx"], ny=mesh.shape["gy"]),
        mesh=mesh,
        in_specs=(spec, spec, P(), flat, flat),
        out_specs=(spec, spec),
        check_vma=False,
    )
```
